512 devices in a mesh: groups: 2 (over y), patch: 128 (over x, z), sub: 2 (over core).
Axes of the slice: x: 4, y: 2, z: 32, core: 2. Of those that a mesh axis runs over, the one named last changes fastest.
The devices are a block of a 4x8x32 slice.
Arguments:
- block_cols: int32 [1024, 3], P(('groups', 'patch', 'sub')), parts along dimension 0, may hold values from 0 to 511, as said below
- step_tiles: float32 [1024, 3, 128, 128], P(('groups', 'patch', 'sub')), parts along dimension 0, as said below
- mass: float32 [131072], P(('groups', 'patch', 'sub')), parts along dimension 0, as said below
- warm_start: float32 [131072, 128], P(('groups', 'patch', 'sub')), parts along dimension 0, may hold values from -2.5 to 2.5
- source_ids: int32 [256], P('groups'), parts along dimension 0, may hold values from 0 to 65535
Outputs:
- solution: float32 [131072, 128], P(('groups', 'patch', 'sub')), parts along dimension 0
The draws below stay inside these ranges and needn't reach their ends.
There are 2 independent parts, one for each index of `groups`. The reference program is written for one: setup_inputs(seed, part) draws one part's arguments, and reference() takes and returns one part's arrays. A program takes and returns all parts, laid end to end along the dimension named above; each array names one. Nothing has to cross between parts.
Inputs may be any that keep to these rules, and one draw needn't show every extreme that they name: `block_cols`: slot lists of block row g name g itself and blocks within 1 of g coupled to it; coupling is symmetric (g names h exactly when h names g). Unused slots name g and carry a zero tile. `step_tiles`: entries are not negative. The tile of block row h toward g is the transpose of the tile of row g toward h; the tile of a row toward itself is symmetric with a zero diagonal. `mass`: between 0.1 and 1.2.
All inputs are finite; a program needn't handle non-finite values.
Results may differ from the reference program's by a relative error of at most 0.00023.
Values sent between devices are 32-bit elements; how exact they have to be, the bound alone decides.
A program may use at most 64 MiB of HBM per device.

```python
import jax
import jax.numpy as jnp
from jax import lax

TILE = 128
REACH = 1
SOURCES = 128
ITERS = 2
BLOCKS = 512
VERTICES = 65536
N_PATCH = 128
N_SUB = 2


def coupling_parts(key):
    key_present, key_upper, key_own = jax.random.split(jax.random.fold_in(key, 11), 3)
    count = BLOCKS
    rows_ids = jnp.arange(count, dtype=jnp.int32)
    ceiling = 8.0 / (TILE * (1.0 + 1.5 * REACH))
    offsets_up = jnp.arange(1, REACH + 1, dtype=jnp.int32)
    present = (jax.random.randint(key_present, (count, REACH), 0, 4) < 3) & (rows_ids[:, None] + offsets_up[None, :] < count)

    def values_of(subkey, shape):
        uniform_part = jax.random.uniform(subkey, shape, jnp.float32)
        return ceiling * uniform_part
    upper = values_of(key_upper, (count, REACH, TILE, TILE))
    own_tile = values_of(key_own, (count, TILE, TILE))
    own_tile = 0.5 * (own_tile + jnp.swapaxes(own_tile, 1, 2)) * (1.0 - jnp.eye(TILE, dtype=jnp.float32))
    tile_list = []
    col_list = []
    live_list = []
    for offset in range(-REACH, REACH + 1):
        if offset == 0:
            live = jnp.ones((count,), dtype=bool)
            tile_now = own_tile
            col_now = rows_ids
        elif offset > 0:
            live = present[:, offset - 1]
            tile_now = upper[:, offset - 1]
            col_now = rows_ids + offset
        else:
            depth = -offset
            live = jnp.concatenate([jnp.zeros((depth,), dtype=bool), present[:count - depth, depth - 1]])
            tile_now = jnp.concatenate([jnp.zeros((depth, TILE, TILE), jnp.float32), jnp.swapaxes(upper[:count - depth, depth - 1], 1, 2)], axis=0)
            col_now = rows_ids - depth
        tile_list.append(jnp.where(live[:, None, None], tile_now, 0.0))
        col_list.append(jnp.where(live, col_now, rows_ids).astype(jnp.int32))
        live_list.append(live)
    slot_count = 2 * REACH + 1
    tiles_all = jnp.stack(tile_list, axis=1)
    cols_all = jnp.stack(col_list, axis=1)
    live_all = jnp.stack(live_list, axis=1)
    scores = (1 - live_all.astype(jnp.int32)) * slot_count + jnp.arange(slot_count, dtype=jnp.int32)[None, :]
    order = jnp.argsort(scores, axis=1, stable=True).astype(jnp.int32)
    cols_all = jnp.take_along_axis(cols_all, order, axis=1)
    tiles_all = jnp.take_along_axis(tiles_all, order[:, :, None, None], axis=1)
    return (cols_all, tiles_all)


def draw_block_cols(key, part):
    return coupling_parts(key)[0]


def draw_step_tiles(key, part):
    return coupling_parts(key)[1]


def draw_mass(key, part):
    subkey = jax.random.fold_in(key, 23)
    fraction = jnp.arange(VERTICES, dtype=jnp.float32) / VERTICES
    ramp = 1.0 + 2.0 * fraction
    base = jnp.exp(jax.random.uniform(subkey, (VERTICES,), jnp.float32, jnp.log(0.1), jnp.log(0.4)))
    return ramp * base


def with_ends(values, rng, low, high):
    shape = values.shape
    spot = [jax.random.randint(jax.random.fold_in(rng, axis), (), 0, shape[axis]) for axis in range(len(shape))]
    values = values.at[tuple(spot)].set(low)
    longest = shape.index(max(shape))
    spot[longest] = (spot[longest] + 1) % shape[longest]
    return values.at[tuple(spot)].set(high)


def shard_levels(rng, shape, cuts, least, top_value):
    def one(position, blocks):
        draws = jax.random.uniform(jax.random.fold_in(jax.random.fold_in(rng, 6), position), (blocks,), jnp.float32, least / len(cuts), top_value / len(cuts))
        return jnp.repeat(jnp.exp(draws), shape[position] // blocks).reshape((-1,) + (1,) * (len(shape) - position - 1))

    level = one(*cuts[0])
    for cut in cuts[1:]:
        level = level * one(*cut)
    return level


def scatter_about(own_key, extent, spread, bound, cuts=(), kind=jnp.bfloat16):
    entries = jax.random.normal(own_key, extent, jnp.float32) * spread
    if len(cuts) > 0:
        entries = shard_levels(own_key, extent, cuts, -0.22, 0.18) * entries
    return jnp.clip(entries, min=-bound, max=bound).astype(kind)


def setup_inputs(seed: int = 0, part: int = 0) -> dict:
    keys = jax.random.split(jax.random.key(seed), 6)
    part_keys = jax.random.split(jax.random.fold_in(keys[5], part), 6)
    block_cols = draw_block_cols(jax.random.fold_in(jax.random.fold_in(keys[5], part), 71), part)
    step_tiles = draw_step_tiles(jax.random.fold_in(jax.random.fold_in(keys[5], part), 71), part)
    mass = draw_mass(jax.random.fold_in(jax.random.fold_in(keys[5], part), 71), part)
    warm_start = scatter_about(part_keys[3], (VERTICES, SOURCES), 0.3, 2.5, ((0, 256),), jnp.float32)
    source_ids = with_ends(jax.random.randint(part_keys[4], (SOURCES,), 0, VERTICES), jax.random.fold_in(part_keys[4], 1), 0, VERTICES - 1).astype(jnp.int32)
    return dict(block_cols=block_cols, step_tiles=step_tiles, mass=mass, warm_start=warm_start, source_ids=source_ids)


def apply_operator(operand, block_cols, step_tiles, diag_total):
    tile_size = step_tiles.shape[-1]
    sources = operand.shape[1]
    padding = jnp.zeros((REACH * tile_size, sources), operand.dtype)
    blocks = jnp.concatenate([padding, operand, padding], axis=0).reshape(-1, tile_size, sources)
    groups_count = N_PATCH * N_SUB
    cols_grouped = block_cols.reshape(groups_count, -1, block_cols.shape[1])
    tiles_grouped = step_tiles.reshape(groups_count, -1, step_tiles.shape[1], tile_size, tile_size)

    def one_group(pieces):
        cols_group, tiles_group = pieces
        picked = blocks[cols_group + REACH]
        return jnp.einsum("bkij,bkjs->bis", tiles_group, picked, precision=lax.Precision.HIGHEST, preferred_element_type=jnp.float32)

    coupled = lax.map(one_group, (cols_grouped, tiles_grouped))
    return diag_total * operand - coupled.reshape(operand.shape)


def reference(block_cols, step_tiles, mass, warm_start, source_ids):
    vertex_ids = jnp.arange(warm_start.shape[0], dtype=jnp.int32)
    rhs = (vertex_ids[:, None] == source_ids[None, :]).astype(jnp.float32)
    degree = jnp.sum(step_tiles, axis=(1, 3)).reshape(-1)
    diag_total = (mass + degree)[:, None]
    solution = warm_start
    residual = rhs - apply_operator(warm_start, block_cols, step_tiles, diag_total)
    direction = residual
    norm_now = jnp.sum(residual * residual, axis=0)
    for iteration in range(ITERS):
        image_vec = apply_operator(direction, block_cols, step_tiles, diag_total)
        alpha_step = norm_now / jnp.sum(direction * image_vec, axis=0)
        solution = solution + alpha_step * direction
        residual = residual - alpha_step * image_vec
        if iteration + 1 < ITERS:
            norm_next = jnp.sum(residual * residual, axis=0)
            direction = residual + (norm_next / norm_now) * direction
            norm_now = norm_next
    return solution
```

```python
import functools

import jax
import jax.numpy as jnp
from jax import lax
from jax.experimental import pallas as pl
from jax.experimental.pallas import tpu as pltpu
from jax.sharding import Mesh
from jax.sharding import PartitionSpec as P

NZ = 32
AXES = ("groups", "patch_0", "patch_1", "sub")
MESH = pl.DeviceIdType.MESH
F32, BF16 = jnp.float32, jnp.bfloat16
ANY = pl.BlockSpec(memory_space=pl.ANY)
VMEM = pl.BlockSpec(memory_space=pltpu.VMEM)


def halves(value):
    high = value.astype(BF16)
    return high, (value - high.astype(F32)).astype(BF16)


def pair(value):
    return jnp.concatenate(halves(value), axis=1)


def product(high, low, packed):
    n = packed.shape[1] // 2
    both = jnp.dot(high, packed, preferred_element_type=F32) + jnp.dot(low, packed, preferred_element_type=F32)
    return both[:, :n] + both[:, n:]


def rows_sum(value):
    return jnp.sum(value, axis=0, keepdims=True)


def merged(buf):
    sq, cross, about, rss, quad, lin = (buf[:, k, :] for k in range(6))
    sq_all, cross_all = rows_sum(sq), rows_sum(cross)
    centre = jnp.where(sq_all > 0, cross_all / sq_all, 0.0)
    off = about - centre
    first = cross - about * sq
    rss_all = rows_sum(rss + off * (2.0 * first + off * sq))
    quad_all = rows_sum(quad + off * (lin + off * cross))
    lin_all = rows_sum(lin + 2.0 * off * cross)
    return sq_all, cross_all, centre, rss_all, quad_all, lin_all


def kernel(
    nx, tile,
    cols_h, tiles_h, mass_h, x_h, src_h,
    r_o, w_o, co_o,
    cols, tiles, mass, x, src,
    halo_x, halo_s, halo_w, s_buf, w_buf, own, plane, ranks, plane_sum, total,
    in_sem, x_ss, x_rs, s_ss, s_rs, w_ss, w_rs, p_ss, p_rs, z_ss, z_rs, b_ss, b_rs,
):
    g, px, pz, pc = (lax.axis_index(name) for name in AXES)
    bar = pltpu.get_barrier_semaphore()

    def turn_x(d):
        return lax.rem(px + d + nx, nx)

    def turn_z(d):
        return lax.rem(pz + d + NZ, NZ)

    first, last = pz == 0, pz == NZ - 1
    right = (
        g,
        jnp.where((pc == 1) & last, turn_x(1), px),
        jnp.where(pc == 1, turn_z(1), pz),
        1 - pc,
    )
    left = (
        g,
        jnp.where((pc == 0) & first, turn_x(-1), px),
        jnp.where(pc == 0, turn_z(-1), pz),
        1 - pc,
    )
    far = tuple(jnp.where(pc == 1, a, b) for a, b in zip(right, left))

    def greet(x_at, z_at, c_at):
        pl.semaphore_signal(bar, inc=1, device_id=(g, x_at, z_at, c_at), device_id_type=MESH)

    greet(*far[1:])
    greet(px, pz, 1 - pc)
    for d in range(1, nx):
        for c in range(2):
            greet(turn_x(d), pz, c)

    @pl.when(pc == 1)
    def _():
        greet(px, turn_z(1), pc)
        greet(px, turn_z(-1), pc)

    @pl.when((pc == 1) & first)
    def _():
        for k in range(1, NZ):
            greet(px, k, pc)

    loads = [
        pltpu.make_async_copy(a, b, in_sem.at[i])
        for i, (a, b) in enumerate(((x_h, x), (tiles_h, tiles), (mass_h, mass), (src_h, src), (cols_h, cols)))
    ]
    for load in loads:
        load.start()
    pl.semaphore_wait(bar, 2 * nx + jnp.where(pc == 1, jnp.where(first, 2, 3), 0))

    def send(ref_lo, ref_hi, slots, ss, rs):
        out = [
            pltpu.make_async_remote_copy(ref_hi, slots.at[0], ss.at[0], rs.at[0], device_id=right, device_id_type=MESH),
            pltpu.make_async_remote_copy(ref_lo, slots.at[1], ss.at[1], rs.at[1], device_id=left, device_id_type=MESH),
        ]
        for copy in out:
            copy.start()
        return out

    loads[0].wait()
    sent_x = send(x.at[pl.ds(0, tile)], x.at[pl.ds(tile, tile)], halo_x, x_ss, x_rs)
    for load in loads[1:]:
        load.wait()

    position = (px * NZ + pz) * 2 + pc
    parts = []
    for b in range(2):
        here = position * 2 + b
        found = []
        for d in (-1, 0, 1):
            found.append(sum((cols[b, k] == here + d).astype(F32) * tiles[b, k] for k in range(3)))
        parts.append(found)
    (t0l, t00, t01), (t10, t11, t1r) = parts
    eye = lax.broadcasted_iota(jnp.int32, (tile, tile), 0) == lax.broadcasted_iota(jnp.int32, (tile, tile), 1)
    ones = jnp.ones((tile, tile), BF16)
    diag = []
    for b in range(2):
        row = mass[pl.ds(b * tile, tile)].reshape(1, tile)
        rest = jnp.where(eye, row, 0.0) + (parts[b][0] + parts[b][1] + parts[b][2])
        high = rest.astype(BF16)
        rest = rest - high.astype(F32)
        mid = rest.astype(BF16)
        low = (rest - mid.astype(F32)).astype(BF16)
        diag.append(sum(jnp.dot(part, ones, preferred_element_type=F32) for part in (low, mid, high)))
    diag = jnp.concatenate(diag, axis=0)
    inner = halves(jnp.concatenate([jnp.concatenate([t00, t01], axis=1), jnp.concatenate([t10, t11], axis=1)], axis=0))
    to_left, to_right = halves(t0l), halves(t1r)

    x_pair = pair(x[...])
    ids = lax.broadcasted_iota(jnp.int32, (2 * tile, src.shape[0]), 0) + position * 2 * tile
    rhs = (ids == src[...].reshape(1, -1)).astype(F32)
    s = rhs - diag * x[...] + product(*inner, x_pair)
    s_buf[...] = s
    from_left, from_right = halves(t0l.T), halves(t1r.T)
    sent_s = send(s_buf.at[pl.ds(0, tile)], s_buf.at[pl.ds(tile, tile)], halo_s, s_ss, s_rs)
    on_left = product(*from_left, x_pair[:tile])
    on_right = product(*from_right, x_pair[tile:])

    for copy in sent_x:
        copy.wait()
    r = s + jnp.concatenate([product(*to_left, pair(halo_x[0])), product(*to_right, pair(halo_x[1]))], axis=0)
    r_o[...] = r
    near = diag * r - product(*inner, pair(r))
    for copy in sent_s:
        copy.wait()
    w = near - jnp.concatenate(
        [product(*to_left, pair(halo_s[0] + on_left)), product(*to_right, pair(halo_s[1] + on_right))], axis=0
    )
    w_buf[...] = w
    w_o[...] = w
    sent_w = send(w_buf.at[pl.ds(0, tile)], w_buf.at[pl.ds(tile, tile)], halo_w, w_ss, w_rs)

    sq, cross = rows_sum(r * r), rows_sum(r * w)
    ceiling = 2.0 * jnp.max(diag)
    about = jnp.where(sq > 0, jnp.clip(cross / sq, 0.0, ceiling), 0.0)
    u = w - about * r
    rss = rows_sum(u * u)
    v_near = diag * w - product(*inner, pair(w))
    for copy in sent_w:
        copy.wait()
    v = v_near - jnp.concatenate([product(*to_left, pair(halo_w[0])), product(*to_right, pair(halo_w[1]))], axis=0)
    y = v - about * w
    quad, lin = rows_sum(u * y), rows_sum(u * w + r * y)
    blank = jnp.zeros((2, sq.shape[1]), F32)
    mine = jnp.concatenate([sq, cross, about, rss, quad, lin, blank], axis=0)
    own[...] = mine

    slot = px * 2 + pc
    to_plane = [
        pltpu.make_async_remote_copy(
            own, plane.at[slot], p_ss.at[d], p_rs.at[slot], device_id=(g, turn_x(d), pz, 1), device_id_type=MESH
        )
        for d in range(nx)
    ]
    for copy in to_plane[1:]:
        copy.start()

    @pl.when(pc == 0)
    def _():
        to_plane[0].start()

    down = pltpu.make_async_remote_copy(
        plane_sum, ranks.at[pz], z_ss, z_rs.at[pz], device_id=(g, px, 0, 1), device_id_type=MESH
    )

    def pass_on(c, z_at, k):
        return pltpu.make_async_remote_copy(
            total, total, b_ss.at[k], b_rs, device_id=(g, px, z_at, c), device_id_type=MESH
        )

    half = NZ // 2
    across, up, back = pass_on(0, pz, 0), pass_on(1, turn_z(1), 1), pass_on(1, turn_z(-1), 2)

    @pl.when(pc == 1)
    def _():
        plane[slot] = mine
        for d in range(nx):
            for c in range(2):
                if (d, c) != (0, 1):
                    at = turn_x(d) * 2 + c
                    pltpu.make_async_copy(plane.at[at], plane.at[at], p_rs.at[at]).wait()
        rows = merged(plane)
        joined = jnp.concatenate([*rows, blank], axis=0)

        @pl.when(first)
        def _():
            ranks[0] = joined
            for k in range(1, NZ):
                pltpu.make_async_copy(ranks.at[k], ranks.at[k], z_rs.at[k]).wait()
            sq, cross, _, rss, quad, _ = merged(ranks)
            step = sq / cross
            after = step * step * rss
            ratio = after / sq
            step_next = after / (step * step * quad - ratio * after / step)
            total[...] = jnp.concatenate(
                [step + step_next * (1.0 + ratio), -(step_next * step), jnp.zeros((6, sq.shape[1]), F32)], axis=0
            )

        @pl.when(jnp.logical_not(first))
        def _():
            plane_sum[...] = joined
            down.start()
            pltpu.make_async_copy(total, total, b_rs).wait()

        @pl.when(pz < half)
        def _():
            up.start()

        @pl.when(first | (pz > half + 1))
        def _():
            back.start()

        across.start()

    @pl.when(pc == 0)
    def _():
        pltpu.make_async_copy(total, total, b_rs).wait()

    co_o[...] = total[...]

    for copy in to_plane[1:]:
        copy.wait_send()

    @pl.when(pc == 0)
    def _():
        to_plane[0].wait_send()

    @pl.when(pc == 1)
    def _():
        @pl.when(jnp.logical_not(first))
        def _():
            down.wait_send()

        @pl.when(pz < half)
        def _():
            up.wait_send()

        @pl.when(first | (pz > half + 1))
        def _():
            back.wait_send()

        across.wait_send()


def body(block_cols, step_tiles, mass, warm_start, source_ids):
    nx = lax.axis_size("patch_0")
    tile = step_tiles.shape[-1]
    rows, width = warm_start.shape
    block = (2, tile, width)
    sem = pltpu.SemaphoreType.DMA
    r, w, co = pl.pallas_call(
        functools.partial(kernel, nx, tile),
        out_shape=[
            jax.ShapeDtypeStruct((rows, width), F32),
            jax.ShapeDtypeStruct((rows, width), F32),
            jax.ShapeDtypeStruct((8, width), F32),
        ],
        in_specs=[ANY] * 5,
        out_specs=[VMEM] * 3,
        scratch_shapes=[
            pltpu.SMEM(block_cols.shape, jnp.int32),
            pltpu.VMEM(step_tiles.shape, F32),
            pltpu.VMEM(mass.shape, F32),
            pltpu.VMEM((rows, width), F32),
            pltpu.VMEM(source_ids.shape, jnp.int32),
            pltpu.VMEM(block, F32),
            pltpu.VMEM(block, F32),
            pltpu.VMEM(block, F32),
            pltpu.VMEM((rows, width), F32),
            pltpu.VMEM((rows, width), F32),
            pltpu.VMEM((8, width), F32),
            pltpu.VMEM((2 * nx, 8, width), F32),
            pltpu.VMEM((NZ, 8, width), F32),
            pltpu.VMEM((8, width), F32),
            pltpu.VMEM((8, width), F32),
            sem((5,)),
            sem((2,)), sem((2,)),
            sem((2,)), sem((2,)),
            sem((2,)), sem((2,)),
            sem((nx,)), sem((2 * nx,)),
            sem, sem((NZ,)),
            sem((3,)), sem,
        ],
        compiler_params=pltpu.CompilerParams(collective_id=0, has_side_effects=True),
        name="heat",
    )(block_cols, step_tiles, mass, warm_start, source_ids)
    return warm_start + co[0:1] * r + co[1:2] * w


def solution(mesh):
    split = Mesh(
        mesh.devices.reshape(mesh.shape["groups"], mesh.shape["patch"] // NZ, NZ, mesh.shape["sub"]), AXES
    )
    placed = (P(AXES, None), P(AXES, None, None, None), P(AXES), P(AXES, None), P("groups"))
    return jax.shard_map(body, mesh=split, in_specs=placed, out_specs=P(AXES, None), check_vma=False)
```

```python
import functools

import jax
import jax.numpy as jnp
from jax import lax
from jax.experimental import pallas as pl
from jax.experimental.pallas import tpu as pltpu
from jax.sharding import Mesh
from jax.sharding import PartitionSpec as P

NZ = 32
DIRECT = 3
AXES = ("groups", "patch_0", "patch_1", "sub")
MESH = pl.DeviceIdType.MESH
F32, BF16 = jnp.float32, jnp.bfloat16
ANY = pl.BlockSpec(memory_space=pl.ANY)


def halves(value):
    high = value.astype(BF16)
    return high, (value - high.astype(F32)).astype(BF16)


def pair(value):
    return jnp.concatenate(halves(value), axis=1)


def product(high, low, packed):
    n = packed.shape[1] // 2
    both = jnp.dot(high, packed, preferred_element_type=F32) + jnp.dot(low, packed, preferred_element_type=F32)
    return both[:, :n] + both[:, n:]


def rows_sum(value):
    return jnp.sum(value, axis=0, keepdims=True)


def merged(buf):
    sq, cross, about, rss, quad, lin, curv = (buf[:, k, :] for k in range(7))
    sq_all, cross_all = rows_sum(sq), rows_sum(cross)
    centre = jnp.where(sq_all > 0, cross_all / sq_all, 0.0)
    off = about - centre
    first = cross - about * sq
    rss_all = rows_sum(rss + off * (2.0 * first + off * sq))
    quad_all = rows_sum(quad + off * (lin + off * curv))
    lin_all = rows_sum(lin + 2.0 * off * curv)
    return sq_all, cross_all, centre, rss_all, quad_all, lin_all, rows_sum(curv)


def kernel(
    nx, tile,
    cols_h, tiles_h, mass_h, x_h, src_h,
    out,
    cols, tiles, mass, x, src,
    halo_x, halo_s, halo_w, halo_m, halo_q, s_buf, w_buf, m_buf, q_buf, own, ranks, plane_sum, total,
    in_sem, x_ss, x_rs, s_ss, s_rs, w_ss, w_rs, m_ss, m_rs, q_ss, q_rs, p_ss, z_ss, z_rs, b_ss, b_rs,
):
    g, px, pz, pc = (lax.axis_index(name) for name in AXES)
    bar = pltpu.get_barrier_semaphore()

    def turn_x(d):
        return lax.rem(px + d + nx, nx)

    def turn_z(d):
        return lax.rem(pz + d + NZ, NZ)

    first, last = pz == 0, pz == NZ - 1
    right = (
        g,
        jnp.where((pc == 1) & last, turn_x(1), px),
        jnp.where(pc == 1, turn_z(1), pz),
        1 - pc,
    )
    left = (
        g,
        jnp.where((pc == 0) & first, turn_x(-1), px),
        jnp.where(pc == 0, turn_z(-1), pz),
        1 - pc,
    )
    far = tuple(jnp.where(pc == 1, a, b) for a, b in zip(right, left))
    partner = (g, px, pz, 1 - pc)
    direct = pz >= NZ - DIRECT

    def greet(x_at, z_at, c_at):
        pl.semaphore_signal(bar, inc=1, device_id=(g, x_at, z_at, c_at), device_id_type=MESH)

    greet(*far[1:])
    greet(px, pz, 1 - pc)
    for d in range(1, nx):
        for c in range(2):
            greet(turn_x(d), pz, c)

    @pl.when(pc == 1)
    def _():
        greet(px, turn_z(1), pc)
        greet(px, turn_z(-1), pc)

    @pl.when((pc == 1) & first)
    def _():
        for k in range(1, NZ):
            if k < NZ - DIRECT:
                greet(px, k, 1)
            else:
                for d in range(nx):
                    for c in range(2):
                        greet(turn_x(d), k, c)

    loads = [
        pltpu.make_async_copy(a, b, in_sem.at[i])
        for i, (a, b) in enumerate(((x_h, x), (tiles_h, tiles), (mass_h, mass), (src_h, src), (cols_h, cols)))
    ]
    for load in loads:
        load.start()
    from_roots = jnp.where(direct, nx, jnp.where((pc == 1) & jnp.logical_not(first), 1, 0))
    pl.semaphore_wait(bar, 2 * nx + jnp.where(pc == 1, 2, 0) + from_roots)

    def send(src, dst, ss, rs, to):
        copy = pltpu.make_async_remote_copy(src, dst, ss, rs, device_id=to, device_id_type=MESH)
        copy.start()
        return copy

    def landed(ref, sem):
        pltpu.make_async_copy(ref, ref, sem).wait()

    loads[0].wait()
    sent = [
        send(x.at[pl.ds(0, tile)], halo_x.at[1], x_ss.at[1], x_rs.at[1], left),
        send(x.at[pl.ds(tile, tile)], halo_x.at[0], x_ss.at[0], x_rs.at[0], right),
    ]
    for load in loads[1:]:
        load.wait()

    position = (px * NZ + pz) * 2 + pc
    parts = []
    for b in range(2):
        here = position * 2 + b
        found = []
        for d in (-1, 0, 1):
            found.append(sum((cols[b, k] == here + d).astype(F32) * tiles[b, k] for k in range(3)))
        parts.append(found)
    (t0l, t00, t01), (t10, t11, t1r) = parts
    eye = lax.broadcasted_iota(jnp.int32, (tile, tile), 0) == lax.broadcasted_iota(jnp.int32, (tile, tile), 1)
    ones = jnp.ones((tile, tile), BF16)
    diag = []
    for b in range(2):
        row = mass[pl.ds(b * tile, tile)].reshape(1, tile)
        rest = jnp.where(eye, row, 0.0) + (parts[b][0] + parts[b][1] + parts[b][2])
        high = rest.astype(BF16)
        rest = rest - high.astype(F32)
        mid = rest.astype(BF16)
        low = (rest - mid.astype(F32)).astype(BF16)
        diag.append(sum(jnp.dot(part, ones, preferred_element_type=F32) for part in (low, mid, high)))
    diag_first = diag[0]
    diag = jnp.concatenate(diag, axis=0)
    inner = halves(jnp.concatenate([jnp.concatenate([t00, t01], axis=1), jnp.concatenate([t10, t11], axis=1)], axis=0))
    to_left, to_right = halves(t0l), halves(t1r)

    x_pair = pair(x[...])
    ids = lax.broadcasted_iota(jnp.int32, (2 * tile, src.shape[0]), 0) + position * 2 * tile
    rhs = (ids == src[...].reshape(1, -1)).astype(F32)
    s = rhs - diag * x[...] + product(*inner, x_pair)
    s_buf[0] = s[:tile]
    s_buf[1] = s[tile:]
    m_buf[...] = jnp.where(eye, diag_first, 0.0) - t00
    from_left, from_right = halves(t0l.T), halves(t1r.T)
    sent += [
        send(s_buf.at[0], halo_s.at[1], s_ss.at[1], s_rs.at[1], left),
        send(s_buf.at[1], halo_s.at[0], s_ss.at[0], s_rs.at[0], right),
    ]
    to_chip = [
        pltpu.make_async_remote_copy(m_buf, halo_m, m_ss, m_rs, device_id=left, device_id_type=MESH),
        pltpu.make_async_remote_copy(q_buf, halo_q, q_ss, q_rs, device_id=left, device_id_type=MESH),
    ]

    @pl.when(pc == 0)
    def _():
        to_chip[0].start()
        landed(halo_x.at[1], x_rs.at[1])
        ahead = s[tile:] + product(*to_right, pair(halo_x[1]))
        whole = jnp.concatenate([s[:tile], ahead], axis=0)
        q_buf[...] = diag_first * s[:tile] - product(inner[0][:tile], inner[1][:tile], pair(whole))
        to_chip[1].start()

    on_left = product(*from_left, x_pair[:tile])
    on_right = product(*from_right, x_pair[tile:])

    @pl.when(pc == 1)
    def _():
        landed(halo_x.at[1], x_rs.at[1])

    landed(halo_x.at[0], x_rs.at[0])
    r = s + jnp.concatenate([product(*to_left, pair(halo_x[0])), product(*to_right, pair(halo_x[1]))], axis=0)
    r_pair = pair(r)
    near_r = diag * r - product(*inner, r_pair)
    back_r = [product(*from_left, r_pair[:tile]), product(*from_right, r_pair[tile:])]
    landed(halo_s.at[0], s_rs.at[0])
    landed(halo_s.at[1], s_rs.at[1])
    next_r = [halo_s[0] + on_left, halo_s[1] + on_right]
    w = near_r - jnp.concatenate([product(*to_left, pair(next_r[0])), product(*to_right, pair(next_r[1]))], axis=0)
    w_buf[0] = w[:tile]
    w_buf[1] = w[tile:]
    sent.append(send(w_buf.at[1 - pc], halo_w.at[pc], w_ss, w_rs, partner))

    w_pair = pair(w)
    sq, cross = rows_sum(r * r), rows_sum(r * w)
    ceiling = 2.0 * jnp.max(diag)
    about = jnp.where(sq > 0, jnp.clip(cross / sq, 0.0, ceiling), 0.0)
    u = w - about * r
    rss = rows_sum(u * u)
    near_u = diag * w - product(*inner, w_pair) - about * near_r
    back_u = [
        product(*from_left, w_pair[:tile]) - about * back_r[0],
        product(*from_right, w_pair[tile:]) - about * back_r[1],
    ]
    quad, lin, curv = rows_sum(u * near_u), 2.0 * rows_sum(r * near_u), rows_sum(r * near_r)

    @pl.when(pc == 0)
    def _():
        halo_w[0] = jnp.zeros_like(w_buf[0])

    @pl.when(pc == 1)
    def _():
        landed(halo_m, m_rs)
        across_m = product(*halves(halo_m[...]), pair(on_right)) - back_r[1]
        landed(halo_q, q_rs)
        halo_w[1] = halo_q[...] + across_m

    landed(halo_w.at[1 - pc], w_rs)
    for side, weight in ((0, pc.astype(F32)), (1, 1.0 + pc.astype(F32))):
        next_u = halo_w[side] - about * next_r[side]
        quad -= weight * rows_sum(back_u[side] * next_u)
        lin -= weight * rows_sum(back_u[side] * next_r[side] + back_r[side] * next_u)
        curv -= weight * rows_sum(back_r[side] * next_r[side])
    blank = jnp.zeros((1, sq.shape[1]), F32)
    mine = jnp.concatenate([sq, cross, about, rss, quad, lin, curv, blank], axis=0)
    own[...] = mine

    planes = NZ - DIRECT - 1
    slot = planes + jnp.where(direct, pz - planes, 0) * 2 * nx + px * 2 + pc
    to_plane = [
        pltpu.make_async_remote_copy(
            own, ranks.at[slot], p_ss.at[d], z_rs.at[slot],
            device_id=(g, turn_x(d), jnp.where(direct, 0, pz), 1), device_id_type=MESH,
        )
        for d in range(nx)
    ]
    for copy in to_plane[1:]:
        copy.start()

    @pl.when((pc == 0) | direct)
    def _():
        to_plane[0].start()

    rank = jnp.clip(pz - 1, 0, planes - 1)
    down = pltpu.make_async_remote_copy(
        plane_sum, ranks.at[rank], z_ss, z_rs.at[rank], device_id=(g, px, 0, 1), device_id_type=MESH
    )

    def pass_on(c, z_at, k):
        return pltpu.make_async_remote_copy(
            total, total, b_ss.at[k], b_rs, device_id=(g, px, z_at, c), device_id_type=MESH
        )

    half = NZ // 2
    across, up, back = pass_on(0, pz, 0), pass_on(1, turn_z(1), 1), pass_on(1, turn_z(-1), 2)

    @pl.when((pc == 1) & jnp.logical_not(direct))
    def _():
        ranks[slot] = mine
        for d in range(nx):
            for c in range(2):
                if (d, c) != (0, 1):
                    at = planes + turn_x(d) * 2 + c
                    landed(ranks.at[at], z_rs.at[at])

        @pl.when(jnp.logical_not(first))
        def _():
            plane_sum[...] = jnp.concatenate([*merged(ranks.at[pl.ds(planes, 2 * nx)]), blank], axis=0)
            down.start()

    @pl.when((pc == 1) & first)
    def _():
        for k in (*range(planes), *range(planes + 2 * nx, planes + 2 * nx * (DIRECT + 1))):
            landed(ranks.at[k], z_rs.at[k])
        sq, cross, _, rss, quad, _, _ = merged(ranks)
        step = sq / cross
        after = step * step * rss
        ratio = after / sq
        step_next = after / (step * step * quad - ratio * after / step)
        total[...] = jnp.concatenate(
            [step + step_next * (1.0 + ratio), -(step_next * step), jnp.zeros((6, sq.shape[1]), F32)], axis=0
        )

    @pl.when(jnp.logical_not((pc == 1) & first))
    def _():
        landed(total, b_rs)

    go_up, go_back = (pc == 1) & (pz < half), (pc == 1) & (first | (pz > half + 1))

    @pl.when(pc == 1)
    def _():
        across.start()

    @pl.when(go_up)
    def _():
        up.start()

    @pl.when(go_back)
    def _():
        back.start()

    out[...] = x[...] + total[0:1] * r + total[1:2] * w

    for copy in (*sent, *to_plane[1:]):
        copy.wait_send()

    for cond, copies in (
        (pc == 0, to_chip),
        ((pc == 0) | direct, to_plane[:1]),
        ((pc == 1) & jnp.logical_not(direct | first), [down]),
        (pc == 1, [across]),
        (go_up, [up]),
        (go_back, [back]),
    ):

        @pl.when(cond)
        def _(copies=copies):
            for copy in copies:
                copy.wait_send()


def body(block_cols, step_tiles, mass, warm_start, source_ids):
    nx = lax.axis_size("patch_0")
    tile = step_tiles.shape[-1]
    rows, width = warm_start.shape
    edge, square, sums = (2, tile, width), (tile, tile), (8, width)
    slots = NZ - DIRECT - 1 + 2 * nx * (DIRECT + 1)
    sem = pltpu.SemaphoreType.DMA
    return pl.pallas_call(
        functools.partial(kernel, nx, tile),
        out_shape=pltpu.VMEM((rows, width), F32),
        in_specs=[ANY] * 5,
        out_specs=pl.BlockSpec(memory_space=pltpu.VMEM),
        scratch_shapes=[
            pltpu.SMEM(block_cols.shape, jnp.int32),
            pltpu.VMEM(step_tiles.shape, F32),
            pltpu.VMEM(mass.shape, F32),
            pltpu.VMEM((rows, width), F32),
            pltpu.VMEM(source_ids.shape, jnp.int32),
            pltpu.VMEM(edge, F32), pltpu.VMEM(edge, F32), pltpu.VMEM(edge, F32),
            pltpu.VMEM(square, F32), pltpu.VMEM((tile, width), F32),
            pltpu.VMEM(edge, F32), pltpu.VMEM(edge, F32),
            pltpu.VMEM(square, F32), pltpu.VMEM((tile, width), F32),
            pltpu.VMEM(sums, F32),
            pltpu.VMEM((slots, *sums), F32),
            pltpu.VMEM(sums, F32),
            pltpu.VMEM(sums, F32),
            sem((5,)),
            sem((2,)), sem((2,)),
            sem((2,)), sem((2,)),
            sem, sem,
            sem, sem,
            sem, sem,
            sem((nx,)),
            sem, sem((slots,)),
            sem((3,)), sem,
        ],
        compiler_params=pltpu.CompilerParams(collective_id=0, has_side_effects=True),
        name="heat",
    )(block_cols, step_tiles, mass, warm_start, source_ids)


def solution(mesh):
    split = Mesh(
        mesh.devices.reshape(mesh.shape["groups"], mesh.shape["patch"] // NZ, NZ, mesh.shape["sub"]), AXES
    )
    placed = (P(AXES, None), P(AXES, None, None, None), P(AXES), P(AXES, None), P("groups"))
    return jax.shard_map(body, mesh=split, in_specs=placed, out_specs=P(AXES, None), check_vma=False)
```

```python
import functools

import jax
import jax.numpy as jnp
from jax import lax
from jax.experimental import pallas as pl
from jax.experimental.pallas import tpu as pltpu
from jax.sharding import Mesh
from jax.sharding import PartitionSpec as P

NZ = 32
AXES = ("groups", "patch_0", "patch_1", "sub")
MESH = pl.DeviceIdType.MESH
F32, BF16 = jnp.float32, jnp.bfloat16
ANY = pl.BlockSpec(memory_space=pl.ANY)


def halves(value):
    high = value.astype(BF16)
    return high, (value - high.astype(F32)).astype(BF16)


def pair(value):
    return jnp.concatenate(halves(value), axis=1)


def product(high, low, packed):
    n = packed.shape[1] // 2
    both = jnp.dot(high, packed, preferred_element_type=F32) + jnp.dot(low, packed, preferred_element_type=F32)
    return both[:, :n] + both[:, n:]


def rows_sum(value):
    return jnp.sum(value, axis=0, keepdims=True)


def merged(buf):
    sq, cross, about, rss, quad, lin, curv = (buf[:, k, :] for k in range(7))
    sq_all, cross_all = rows_sum(sq), rows_sum(cross)
    centre = jnp.where(sq_all > 0, cross_all / sq_all, 0.0)
    off = about - centre
    first = cross - about * sq
    rss_all = rows_sum(rss + off * (2.0 * first + off * sq))
    quad_all = rows_sum(quad + off * (lin + off * curv))
    lin_all = rows_sum(lin + 2.0 * off * curv)
    return sq_all, cross_all, centre, rss_all, quad_all, lin_all, rows_sum(curv)


def kernel(
    nx, tile,
    cols_h, tiles_h, mass_h, x_h, src_h,
    out,
    cols, tiles, mass, x, src,
    halo_x, halo_s, halo_w, halo_m, halo_q, s_buf, w_buf, m_buf, q_buf, own, ranks, line, lines, total,
    in_sem, x_ss, x_rs, s_ss, s_rs, w_ss, w_rs, m_ss, m_rs, q_ss, q_rs, z_ss, z_rs, l_ss, l_rs, b_ss, b_rs,
):
    g, px, pz, pc = (lax.axis_index(name) for name in AXES)
    bar = pltpu.get_barrier_semaphore()

    def turn_x(d):
        return lax.rem(px + d + nx, nx)

    def turn_z(d):
        return lax.rem(pz + d + NZ, NZ)

    first, last = pz == 0, pz == NZ - 1
    right = (
        g,
        jnp.where((pc == 1) & last, turn_x(1), px),
        jnp.where(pc == 1, turn_z(1), pz),
        1 - pc,
    )
    left = (
        g,
        jnp.where((pc == 0) & first, turn_x(-1), px),
        jnp.where(pc == 0, turn_z(-1), pz),
        1 - pc,
    )
    far = tuple(jnp.where(pc == 1, a, b) for a, b in zip(right, left))
    partner = (g, px, pz, 1 - pc)
    is_root = first & (pc == 1)

    loads = [
        pltpu.make_async_copy(a, b, in_sem.at[i])
        for i, (a, b) in enumerate(((x_h, x), (tiles_h, tiles), (mass_h, mass), (src_h, src), (cols_h, cols)))
    ]
    for load in loads:
        load.start()

    def greet(x_at, z_at, c_at):
        pl.semaphore_signal(bar, inc=1, device_id=(g, x_at, z_at, c_at), device_id_type=MESH)

    greet(*partner[1:])
    greet(*far[1:])

    @pl.when(is_root)
    def _():
        for d in range(1, nx):
            greet(turn_x(d), pz, 1)

        def greet_line(k, carry):
            greet(px, NZ - k, 0)
            greet(px, NZ - k, 1)
            return carry

        lax.fori_loop(1, NZ, greet_line, 0)

    pl.semaphore_wait(bar, 2 + jnp.where(is_root, nx - 1, jnp.where(first, 0, 1)))

    def send(src, dst, ss, rs, to):
        copy = pltpu.make_async_remote_copy(src, dst, ss, rs, device_id=to, device_id_type=MESH)
        copy.start()
        return copy

    def landed(ref, sem):
        pltpu.make_async_copy(ref, ref, sem).wait()

    loads[0].wait()
    sent = [
        send(x.at[pl.ds(0, tile)], halo_x.at[1], x_ss.at[1], x_rs.at[1], left),
        send(x.at[pl.ds(tile, tile)], halo_x.at[0], x_ss.at[0], x_rs.at[0], right),
    ]
    for load in loads[1:]:
        load.wait()

    position = (px * NZ + pz) * 2 + pc
    parts = []
    for b in range(2):
        here = position * 2 + b
        found = []
        for d in (-1, 0, 1):
            found.append(sum((cols[b, k] == here + d).astype(F32) * tiles[b, k] for k in range(3)))
        parts.append(found)
    (t0l, t00, t01), (t10, t11, t1r) = parts
    eye = lax.broadcasted_iota(jnp.int32, (tile, tile), 0) == lax.broadcasted_iota(jnp.int32, (tile, tile), 1)
    ones = jnp.ones((tile, tile), BF16)
    diag = []
    for b in range(2):
        row = mass[pl.ds(b * tile, tile)].reshape(1, tile)
        rest = jnp.where(eye, row, 0.0) + (parts[b][0] + parts[b][1] + parts[b][2])
        high = rest.astype(BF16)
        rest = rest - high.astype(F32)
        mid = rest.astype(BF16)
        low = (rest - mid.astype(F32)).astype(BF16)
        diag.append(sum(jnp.dot(part, ones, preferred_element_type=F32) for part in (low, mid, high)))
    diag_last = diag[1]
    diag = jnp.concatenate(diag, axis=0)
    inner = halves(jnp.concatenate([jnp.concatenate([t00, t01], axis=1), jnp.concatenate([t10, t11], axis=1)], axis=0))
    to_left, to_right = halves(t0l), halves(t1r)

    x_pair = pair(x[...])
    ids = lax.broadcasted_iota(jnp.int32, (2 * tile, src.shape[0]), 0) + position * 2 * tile
    rhs = (ids == src[...].reshape(1, -1)).astype(F32)
    s = rhs - diag * x[...] + product(*inner, x_pair)
    s_buf[0] = s[:tile]
    s_buf[1] = s[tile:]
    m_buf[...] = jnp.where(eye, diag_last, 0.0) - t11
    from_left, from_right = halves(t0l.T), halves(t1r.T)
    sent += [
        send(s_buf.at[0], halo_s.at[1], s_ss.at[1], s_rs.at[1], left),
        send(s_buf.at[1], halo_s.at[0], s_ss.at[0], s_rs.at[0], right),
    ]
    to_chip = [
        pltpu.make_async_remote_copy(m_buf, halo_m, m_ss, m_rs, device_id=right, device_id_type=MESH),
        pltpu.make_async_remote_copy(q_buf, halo_q, q_ss, q_rs, device_id=right, device_id_type=MESH),
    ]

    @pl.when(pc == 1)
    def _():
        to_chip[0].start()
        landed(halo_x.at[0], x_rs.at[0])
        behind = s[:tile] + product(*to_left, pair(halo_x[0]))
        whole = jnp.concatenate([behind, s[tile:]], axis=0)
        q_buf[...] = diag_last * s[tile:] - product(inner[0][tile:], inner[1][tile:], pair(whole))
        to_chip[1].start()

    on_left = product(*from_left, x_pair[:tile])
    on_right = product(*from_right, x_pair[tile:])

    @pl.when(pc == 0)
    def _():
        landed(halo_x.at[0], x_rs.at[0])

    landed(halo_x.at[1], x_rs.at[1])
    r = s + jnp.concatenate([product(*to_left, pair(halo_x[0])), product(*to_right, pair(halo_x[1]))], axis=0)
    r_pair = pair(r)
    near_r = diag * r - product(*inner, r_pair)
    back_r = product(*from_left, r_pair[:tile])
    landed(halo_s.at[0], s_rs.at[0])
    landed(halo_s.at[1], s_rs.at[1])
    next_r = [halo_s[0] + on_left, halo_s[1] + on_right]
    w = near_r - jnp.concatenate([product(*to_left, pair(next_r[0])), product(*to_right, pair(next_r[1]))], axis=0)
    to_core = pltpu.make_async_remote_copy(
        w_buf, halo_w, w_ss, w_rs, device_id=partner, device_id_type=MESH
    )

    @pl.when(pc == 0)
    def _():
        w_buf[...] = w[tile:]
        to_core.start()


    w_pair = pair(w)
    sq, cross = rows_sum(r * r), rows_sum(r * w)
    ceiling = 2.0 * jnp.max(diag)
    about = jnp.where(sq > 0, jnp.clip(cross / sq, 0.0, ceiling), 0.0)
    u = w - about * r
    rss = rows_sum(u * u)
    near_u = diag * w - product(*inner, w_pair) - about * near_r
    back_u = product(*from_left, w_pair[:tile]) - about * back_r
    quad, lin, curv = rows_sum(u * near_u), 2.0 * rows_sum(r * near_u), rows_sum(r * near_r)

    @pl.when(pc == 0)
    def _():
        landed(halo_m, m_rs)
        across_m = product(*halves(halo_m[...]), pair(on_left)) - back_r
        landed(halo_q, q_rs)
        halo_w[...] = halo_q[...] + across_m

    @pl.when(pc == 1)
    def _():
        landed(halo_w, w_rs)

    next_u = halo_w[...] - about * next_r[0]
    quad -= 2.0 * rows_sum(back_u * next_u)
    lin -= 2.0 * rows_sum(back_u * next_r[0] + back_r * next_u)
    curv -= 2.0 * rows_sum(back_r * next_r[0])
    blank = jnp.zeros((1, sq.shape[1]), F32)
    mine = jnp.concatenate([sq, cross, about, rss, quad, lin, curv, blank], axis=0)
    own[...] = mine

    slot = pz * 2 + pc
    to_root = pltpu.make_async_remote_copy(
        own, ranks.at[slot], z_ss, z_rs.at[slot], device_id=(g, px, 0, 1), device_id_type=MESH
    )
    to_lines = [
        pltpu.make_async_remote_copy(
            line, lines.at[px], l_ss.at[d], l_rs.at[px], device_id=(g, turn_x(d), pz, 1), device_id_type=MESH
        )
        for d in range(1, nx)
    ]
    to_partner = pltpu.make_async_remote_copy(
        total, total, b_ss.at[0], b_rs, device_id=partner, device_id_type=MESH
    )

    def to_all(k, act):
        for c in range(2):
            act(
                pltpu.make_async_remote_copy(
                    total, total, b_ss.at[2 * k + c], b_rs, device_id=(g, px, k, c), device_id_type=MESH
                )
            )

    def along(act):
        def step(k, carry):
            to_all(k, act)
            to_all(NZ - k, act)
            return carry

        lax.fori_loop(1, NZ // 2, step, 0)
        to_all(NZ // 2, act)

    @pl.when(is_root)
    def _():
        ranks[1] = mine
        for k in range(2 * NZ):
            if k != 1:
                landed(ranks.at[k], z_rs.at[k])
        joined = jnp.concatenate([*merged(ranks), blank], axis=0)
        line[...] = joined
        lines[px] = joined
        for copy in to_lines:
            copy.start()
        for d in range(1, nx):
            landed(lines.at[turn_x(d)], l_rs.at[turn_x(d)])
        sq, cross, _, rss, quad, _, _ = merged(lines)
        step = sq / cross
        after = step * step * rss
        ratio = after / sq
        step_next = after / (step * step * quad - ratio * after / step)
        total[...] = jnp.concatenate([step + step_next * (1.0 + ratio), -(step_next * step)], axis=0)
        to_partner.start()

    @pl.when(jnp.logical_not(is_root))
    def _():
        to_root.start()
        landed(total, b_rs)

    is_caster = first & (pc == 0)

    @pl.when(is_caster)
    def _():
        along(lambda copy: copy.start())

    out[...] = x[...] + total[0:1] * r + total[1:2] * w

    for copy in sent:
        copy.wait_send()

    @pl.when(pc == 0)
    def _():
        to_core.wait_send()

    @pl.when(pc == 1)
    def _():
        for copy in to_chip:
            copy.wait_send()

    @pl.when(is_root)
    def _():
        for copy in (*to_lines, to_partner):
            copy.wait_send()

    @pl.when(jnp.logical_not(is_root))
    def _():
        to_root.wait_send()

    @pl.when(is_caster)
    def _():
        along(lambda copy: copy.wait_send())


def body(block_cols, step_tiles, mass, warm_start, source_ids):
    nx = lax.axis_size("patch_0")
    tile = step_tiles.shape[-1]
    rows, width = warm_start.shape
    edge, square, sums = (2, tile, width), (tile, tile), (8, width)
    sem = pltpu.SemaphoreType.DMA
    return pl.pallas_call(
        functools.partial(kernel, nx, tile),
        out_shape=pltpu.VMEM((rows, width), F32),
        in_specs=[ANY] * 5,
        out_specs=pl.BlockSpec(memory_space=pltpu.VMEM),
        scratch_shapes=[
            pltpu.SMEM(block_cols.shape, jnp.int32),
            pltpu.VMEM(step_tiles.shape, F32),
            pltpu.VMEM(mass.shape, F32),
            pltpu.VMEM((rows, width), F32),
            pltpu.VMEM(source_ids.shape, jnp.int32),
            pltpu.VMEM(edge, F32), pltpu.VMEM(edge, F32), pltpu.VMEM(edge[1:], F32),
            pltpu.VMEM(square, F32), pltpu.VMEM(edge[1:], F32),
            pltpu.VMEM(edge, F32), pltpu.VMEM(edge[1:], F32),
            pltpu.VMEM(square, F32), pltpu.VMEM(edge[1:], F32),
            pltpu.VMEM(sums, F32),
            pltpu.VMEM((2 * NZ, *sums), F32),
            pltpu.VMEM(sums, F32),
            pltpu.VMEM((nx, *sums), F32),
            pltpu.VMEM((2, width), F32),
            sem((5,)),
            sem((2,)), sem((2,)),
            sem((2,)), sem((2,)),
            sem, sem,
            sem, sem,
            sem, sem,
            sem, sem((2 * NZ,)),
            sem((nx,)), sem((nx,)),
            sem((2 * NZ,)), sem,
        ],
        compiler_params=pltpu.CompilerParams(collective_id=0, has_side_effects=True),
        name="heat",
    )(block_cols, step_tiles, mass, warm_start, source_ids)


def solution(mesh):
    split = Mesh(
        mesh.devices.reshape(mesh.shape["groups"], mesh.shape["patch"] // NZ, NZ, mesh.shape["sub"]), AXES
    )
    placed = (P(AXES, None), P(AXES, None, None, None), P(AXES), P(AXES, None), P("groups"))
    return jax.shard_map(body, mesh=split, in_specs=placed, out_specs=P(AXES, None), check_vma=False)
```

```python
import functools

import jax
import jax.numpy as jnp
from jax import lax
from jax.experimental import pallas as pl
from jax.experimental.pallas import tpu as pltpu
from jax.sharding import Mesh
from jax.sharding import PartitionSpec as P

NZ = 32
AXES = ("groups", "patch_0", "patch_1", "sub")
MESH = pl.DeviceIdType.MESH
F32, BF16 = jnp.float32, jnp.bfloat16
ANY = pl.BlockSpec(memory_space=pl.ANY)


def halves(value):
    high = value.astype(BF16)
    return high, (value - high.astype(F32)).astype(BF16)


def pair(value):
    return jnp.concatenate(halves(value), axis=1)


def product(high, low, packed):
    n = packed.shape[1] // 2
    both = jnp.dot(high, packed, preferred_element_type=F32) + jnp.dot(low, packed, preferred_element_type=F32)
    return both[:, :n] + both[:, n:]


def rows_sum(value):
    return jnp.sum(value, axis=0, keepdims=True)


def merged(buf):
    sq, cross, about, rss, quad, lin, curv = (buf[:, k, :] for k in range(7))
    sq_all, cross_all = rows_sum(sq), rows_sum(cross)
    centre = jnp.where(sq_all > 0, cross_all / sq_all, 0.0)
    off = about - centre
    first = cross - about * sq
    rss_all = rows_sum(rss + off * (2.0 * first + off * sq))
    quad_all = rows_sum(quad + off * (lin + off * curv))
    lin_all = rows_sum(lin + 2.0 * off * curv)
    return sq_all, cross_all, centre, rss_all, quad_all, lin_all, rows_sum(curv)


def kernel(
    nx, tile,
    cols_h, tiles_h, mass_h, x_h, src_h,
    out,
    cols, tiles, mass, x, src,
    halo_x, halo_s, halo_w, halo_m, halo_q, s_buf, w_buf, m_buf, q_buf, own, ranks, line, late, total,
    in_sem, x_ss, x_rs, s_ss, s_rs, w_ss, w_rs, m_ss, m_rs, q_ss, q_rs, pass_ss, up_sem,
    z_ss, z_rs, l_ss, l_rs, b_ss, b_rs,
):
    g, px, pz, pc = (lax.axis_index(name) for name in AXES)
    bar = pltpu.get_barrier_semaphore()

    def turn_x(d):
        return lax.rem(px + d + nx, nx)

    def turn_z(d):
        return lax.rem(pz + d + NZ, NZ)

    first, last = pz == 0, pz == NZ - 1
    right = (g, jnp.where((pc == 1) & last, turn_x(1), px), jnp.where(pc == 1, turn_z(1), pz), 1 - pc)
    left = (g, jnp.where((pc == 0) & first, turn_x(-1), px), jnp.where(pc == 0, turn_z(-1), pz), 1 - pc)
    far = tuple(jnp.where(pc == 1, a, b) for a, b in zip(right, left))
    partner = (g, px, pz, 1 - pc)
    is_root, is_caster, is_end = first & (pc == 1), first & (pc == 0), last & (pc == 1)
    by_way = (g, jnp.where(is_caster, turn_x(-1), left[1]), jnp.where(is_caster, 0, left[2]), left[3])
    way_slot = jnp.where(is_caster, 2, 1)

    loads = [
        pltpu.make_async_copy(a, b, in_sem.at[i])
        for i, (a, b) in enumerate(((x_h, x), (tiles_h, tiles), (mass_h, mass), (src_h, src), (cols_h, cols)))
    ]
    for load in loads:
        load.start()

    def greet(x_at, z_at, c_at):
        pl.semaphore_signal(bar, inc=1, device_id=(g, x_at, z_at, c_at), device_id_type=MESH)

    greet(*partner[1:])

    @pl.when(jnp.logical_not(is_end))
    def _():
        greet(*far[1:])

    @pl.when(first)
    def _():
        for d in range(nx):
            for c in range(2):
                greet(turn_x(d), NZ - 1, c)
                if d > 0:
                    greet(turn_x(d), 0, c)

    @pl.when(is_root)
    def _():
        def greet_line(k, carry):
            greet(px, NZ - 1 - k, 0)
            greet(px, NZ - 1 - k, 1)
            return carry

        lax.fori_loop(1, NZ - 1, greet_line, 0)

    mates = 2 * nx - 1
    pl.semaphore_wait(
        bar, jnp.where(first, mates + jnp.where(is_root, 1, 0), jnp.where(last, 2 + 2 * nx, 3))
    )

    def send(src, dst, ss, rs, to):
        copy = pltpu.make_async_remote_copy(src, dst, ss, rs, device_id=to, device_id_type=MESH)
        copy.start()
        return copy

    def landed(ref, sem):
        pltpu.make_async_copy(ref, ref, sem).wait()

    @pl.when(is_end)
    def _():
        pl.semaphore_signal(up_sem, inc=1, device_id=(g, px, 0, 1), device_id_type=MESH)

    loads[0].wait()
    sent = [
        send(x.at[pl.ds(0, tile)], halo_x.at[way_slot], x_ss.at[1], x_rs.at[way_slot], by_way),
        send(x.at[pl.ds(tile, tile)], halo_x.at[0], x_ss.at[0], x_rs.at[0], right),
    ]
    for load in loads[1:]:
        load.wait()

    position = (px * NZ + pz) * 2 + pc
    parts = []
    for b in range(2):
        here = position * 2 + b
        found = []
        for d in (-1, 0, 1):
            found.append(sum((cols[b, k] == here + d).astype(F32) * tiles[b, k] for k in range(3)))
        parts.append(found)
    (t0l, t00, t01), (t10, t11, t1r) = parts
    eye = lax.broadcasted_iota(jnp.int32, (tile, tile), 0) == lax.broadcasted_iota(jnp.int32, (tile, tile), 1)
    ones = jnp.ones((tile, tile), BF16)
    diag = []
    for b in range(2):
        row = mass[pl.ds(b * tile, tile)].reshape(1, tile)
        rest = jnp.where(eye, row, 0.0) + (parts[b][0] + parts[b][1] + parts[b][2])
        high = rest.astype(BF16)
        rest = rest - high.astype(F32)
        mid = rest.astype(BF16)
        low = (rest - mid.astype(F32)).astype(BF16)
        diag.append(sum(jnp.dot(part, ones, preferred_element_type=F32) for part in (low, mid, high)))
    diag_last = diag[1]
    diag = jnp.concatenate(diag, axis=0)
    inner = halves(jnp.concatenate([jnp.concatenate([t00, t01], axis=1), jnp.concatenate([t10, t11], axis=1)], axis=0))
    to_left, to_right = halves(t0l), halves(t1r)

    x_pair = pair(x[...])
    ids = lax.broadcasted_iota(jnp.int32, (2 * tile, src.shape[0]), 0) + position * 2 * tile
    rhs = (ids == src[...].reshape(1, -1)).astype(F32)
    s = rhs - diag * x[...] + product(*inner, x_pair)
    s_buf[0] = s[:tile]
    s_buf[1] = s[tile:]
    m_buf[...] = jnp.where(eye, diag_last, 0.0) - t11
    from_left, from_right = halves(t0l.T), halves(t1r.T)
    sent += [
        send(s_buf.at[0], halo_s.at[way_slot], s_ss.at[1], s_rs.at[way_slot], by_way),
        send(s_buf.at[1], halo_s.at[0], s_ss.at[0], s_rs.at[0], right),
    ]
    to_chip = [
        pltpu.make_async_remote_copy(m_buf, halo_m, m_ss, m_rs, device_id=right, device_id_type=MESH),
        pltpu.make_async_remote_copy(q_buf, halo_q, q_ss, q_rs, device_id=right, device_id_type=MESH),
    ]

    passed = [
        pltpu.make_async_remote_copy(
            ref.at[2], ref.at[1], pass_ss.at[i], rs.at[1], device_id=(g, px, NZ - 1, 1), device_id_type=MESH
        )
        for i, (ref, rs) in enumerate(((halo_x, x_rs), (halo_s, s_rs)))
    ]

    @pl.when(is_root)
    def _():
        landed(halo_x.at[2], x_rs.at[2])
        landed(halo_s.at[2], s_rs.at[2])
        pl.semaphore_wait(up_sem, 1)
        for copy in passed:
            copy.start()

    @pl.when(pc == 1)
    def _():
        to_chip[0].start()
        landed(halo_x.at[0], x_rs.at[0])
        behind = s[:tile] + product(*to_left, pair(halo_x[0]))
        whole = jnp.concatenate([behind, s[tile:]], axis=0)
        q_buf[...] = diag_last * s[tile:] - product(inner[0][tile:], inner[1][tile:], pair(whole))
        to_chip[1].start()

    on_left = product(*from_left, x_pair[:tile])
    on_right = product(*from_right, x_pair[tile:])

    @pl.when(pc == 0)
    def _():
        landed(halo_x.at[0], x_rs.at[0])

    landed(halo_x.at[1], x_rs.at[1])
    r = s + jnp.concatenate([product(*to_left, pair(halo_x[0])), product(*to_right, pair(halo_x[1]))], axis=0)
    r_pair = pair(r)
    near_r = diag * r - product(*inner, r_pair)
    back_r = product(*from_left, r_pair[:tile])
    landed(halo_s.at[0], s_rs.at[0])
    landed(halo_s.at[1], s_rs.at[1])
    next_r = [halo_s[0] + on_left, halo_s[1] + on_right]
    w = near_r - jnp.concatenate([product(*to_left, pair(next_r[0])), product(*to_right, pair(next_r[1]))], axis=0)
    to_core = pltpu.make_async_remote_copy(
        w_buf, halo_w, w_ss, w_rs, device_id=partner, device_id_type=MESH
    )

    @pl.when(pc == 0)
    def _():
        w_buf[...] = w[tile:]
        to_core.start()


    w_pair = pair(w)
    sq, cross = rows_sum(r * r), rows_sum(r * w)
    ceiling = 2.0 * jnp.max(diag)
    about = jnp.where(sq > 0, jnp.clip(cross / sq, 0.0, ceiling), 0.0)
    u = w - about * r
    rss = rows_sum(u * u)
    near_u = diag * w - product(*inner, w_pair) - about * near_r
    back_u = product(*from_left, w_pair[:tile]) - about * back_r
    quad, lin, curv = rows_sum(u * near_u), 2.0 * rows_sum(r * near_u), rows_sum(r * near_r)

    @pl.when(pc == 0)
    def _():
        landed(halo_m, m_rs)
        across_m = product(*halves(halo_m[...]), pair(on_left)) - back_r
        landed(halo_q, q_rs)
        halo_w[...] = halo_q[...] + across_m

    @pl.when(pc == 1)
    def _():
        landed(halo_w, w_rs)

    next_u = halo_w[...] - about * next_r[0]
    quad -= 2.0 * rows_sum(back_u * next_u)
    lin -= 2.0 * rows_sum(back_u * next_r[0] + back_r * next_u)
    curv -= 2.0 * rows_sum(back_r * next_r[0])
    blank = jnp.zeros((1, sq.shape[1]), F32)
    mine = jnp.concatenate([sq, cross, about, rss, quad, lin, curv, blank], axis=0)
    own[...] = mine

    edge_plane = first | last
    slot = jnp.where(edge_plane, nx + jnp.where(first, 2 * nx, 0) + px * 2 + pc, 0)
    rank = jnp.where(edge_plane, 0, (pz - 1) * 2 + pc)
    others = [(d, c) for d in (2, 1, nx - 1, 0) for c in range(2) if (d, c) != (0, 0)]

    def share(src, at, ss, targets):
        return [
            pltpu.make_async_remote_copy(
                src, late.at[at], ss, l_rs, device_id=(g, turn_x(d), 0, lax.rem(pc + c, 2)), device_id_type=MESH
            )
            for d, c in targets
        ]

    mine_out, line_out = share(own, slot, z_ss, others), share(line, px, l_ss, others)
    (mine_down,) = share(own, slot, z_ss, [(0, 0)])
    mine_to_root = pltpu.make_async_remote_copy(
        own, ranks.at[rank], z_ss, z_rs, device_id=(g, px, 0, 1), device_id_type=MESH
    )

    @pl.when(edge_plane)
    def _():
        for copy in mine_out:
            copy.start()

    @pl.when(last)
    def _():
        mine_down.start()

    @pl.when(jnp.logical_not(edge_plane))
    def _():
        mine_to_root.start()

    count = 5 * nx

    @pl.when(is_root)
    def _():
        inner_planes = ranks.at[pl.ds(0, 2 * NZ - 4)]
        landed(inner_planes, z_rs)
        joined = jnp.concatenate([*merged(inner_planes), blank], axis=0)
        line[...] = joined
        for copy in line_out:
            copy.start()
        late[px] = joined
        late[slot] = mine
        landed(late.at[pl.ds(0, count - 2)], l_rs)

    @pl.when(is_caster)
    def _():
        late[slot] = mine
        landed(late.at[pl.ds(0, count - 1)], l_rs)

    def to_line(k):
        return [
            pltpu.make_async_remote_copy(total, total, b_ss, b_rs, device_id=(g, px, k, c), device_id_type=MESH)
            for c in (1, 0)
        ]

    @pl.when(first)
    def _():
        sq, cross, _, rss, quad, _, _ = merged(late)
        step = sq / cross
        after = step * step * rss
        ratio = after / sq
        step_next = after / (step * step * quad - ratio * after / step)
        total[...] = jnp.concatenate(
            [step + step_next * (1.0 + ratio), -(step_next * step), jnp.zeros((6, sq.shape[1]), F32)], axis=0
        )

    @pl.when(jnp.logical_not(first))
    def _():
        landed(total, b_rs)

    @pl.when(is_caster)
    def _():
        def step(k, carry):
            for copy in (*to_line(k), *to_line(NZ - k)):
                copy.start()
            return carry

        lax.fori_loop(1, NZ // 2, step, 0)
        for copy in to_line(NZ // 2):
            copy.start()

    out[...] = x[...] + total[0:1] * r + total[1:2] * w

    for copy in sent:
        copy.wait_send()

    @pl.when(pc == 0)
    def _():
        to_core.wait_send()

    @pl.when(pc == 1)
    def _():
        for copy in to_chip:
            copy.wait_send()

    @pl.when(first)
    def _():
        landed(late.at[pl.ds(0, mates)], z_ss)

    @pl.when(last)
    def _():
        landed(late.at[pl.ds(0, mates + 1)], z_ss)

    @pl.when(jnp.logical_not(edge_plane))
    def _():
        mine_to_root.wait_send()

    @pl.when(is_root)
    def _():
        landed(late.at[pl.ds(0, mates)], l_ss)
        for copy in passed:
            copy.wait_send()

    @pl.when(is_caster)
    def _():
        landed(ranks, b_ss)


def body(block_cols, step_tiles, mass, warm_start, source_ids):
    nx = lax.axis_size("patch_0")
    tile = step_tiles.shape[-1]
    rows, width = warm_start.shape
    edge, slots, square, sums = (2, tile, width), (3, tile, width), (tile, tile), (8, width)
    sem = pltpu.SemaphoreType.DMA
    return pl.pallas_call(
        functools.partial(kernel, nx, tile),
        out_shape=pltpu.VMEM((rows, width), F32),
        in_specs=[ANY] * 5,
        out_specs=pl.BlockSpec(memory_space=pltpu.VMEM),
        scratch_shapes=[
            pltpu.SMEM(block_cols.shape, jnp.int32),
            pltpu.VMEM(step_tiles.shape, F32),
            pltpu.VMEM(mass.shape, F32),
            pltpu.VMEM((rows, width), F32),
            pltpu.VMEM(source_ids.shape, jnp.int32),
            pltpu.VMEM(slots, F32), pltpu.VMEM(slots, F32), pltpu.VMEM(edge[1:], F32),
            pltpu.VMEM(square, F32), pltpu.VMEM(edge[1:], F32),
            pltpu.VMEM(edge, F32), pltpu.VMEM(edge[1:], F32),
            pltpu.VMEM(square, F32), pltpu.VMEM(edge[1:], F32),
            pltpu.VMEM(sums, F32),
            pltpu.VMEM((2 * NZ - 2, *sums), F32),
            pltpu.VMEM(sums, F32),
            pltpu.VMEM((5 * nx, *sums), F32),
            pltpu.VMEM(sums, F32),
            sem((5,)),
            sem((2,)), sem((3,)),
            sem((2,)), sem((3,)),
            sem, sem,
            sem, sem,
            sem, sem,
            sem((2,)), pltpu.SemaphoreType.REGULAR,
            sem, sem,
            sem, sem,
            sem, sem,
        ],
        compiler_params=pltpu.CompilerParams(collective_id=0, has_side_effects=True),
        name="heat",
    )(block_cols, step_tiles, mass, warm_start, source_ids)


def solution(mesh):
    split = Mesh(
        mesh.devices.reshape(mesh.shape["groups"], mesh.shape["patch"] // NZ, NZ, mesh.shape["sub"]), AXES
    )
    placed = (P(AXES, None), P(AXES, None, None, None), P(AXES), P(AXES, None), P("groups"))
    return jax.shard_map(body, mesh=split, in_specs=placed, out_specs=P(AXES, None), check_vma=False)
```

```python
import functools

import jax
import jax.numpy as jnp
from jax import lax
from jax.experimental import pallas as pl
from jax.experimental.pallas import tpu as pltpu
from jax.sharding import Mesh
from jax.sharding import PartitionSpec as P

NZ = 32
NEAR = 4
AXES = ("groups", "patch_0", "patch_1", "sub")
MESH = pl.DeviceIdType.MESH
F32, BF16 = jnp.float32, jnp.bfloat16
ANY = pl.BlockSpec(memory_space=pl.ANY)


def halves(value):
    high = value.astype(BF16)
    return high, (value - high.astype(F32)).astype(BF16)


def pair(value):
    return jnp.concatenate(halves(value), axis=1)


def product(high, low, packed):
    n = packed.shape[1] // 2
    both = jnp.dot(high, packed, preferred_element_type=F32) + jnp.dot(low, packed, preferred_element_type=F32)
    return both[:, :n] + both[:, n:]


def rows_sum(value):
    return jnp.sum(value, axis=0, keepdims=True)


def merged(buf):
    sq, cross, about, rss, quad, lin, curv = (buf[:, k, :] for k in range(7))
    sq_all, cross_all = rows_sum(sq), rows_sum(cross)
    centre = jnp.where(sq_all > 0, cross_all / sq_all, 0.0)
    off = about - centre
    first = cross - about * sq
    rss_all = rows_sum(rss + off * (2.0 * first + off * sq))
    quad_all = rows_sum(quad + off * (lin + off * curv))
    lin_all = rows_sum(lin + 2.0 * off * curv)
    return sq_all, cross_all, centre, rss_all, quad_all, lin_all, rows_sum(curv)


def kernel(
    nx, tile,
    cols_h, tiles_h, mass_h, x_h, src_h,
    out,
    cols, tiles, mass, x, src,
    halo_x, halo_s, halo_w, halo_m, halo_q, s_buf, w_buf, m_buf, q_buf, own, ranks, line, late, total,
    in_sem, x_rs, s_rs, mw_rs, qz_rs, up_sem, l_rs,
):
    large, small, passing = in_sem.at[0], in_sem.at[1], in_sem.at[2]
    g, px, pz, pc = (lax.axis_index(name) for name in AXES)
    bar = pltpu.get_barrier_semaphore()

    def turn_x(d):
        return lax.rem(px + d + nx, nx)

    def turn_z(d):
        return lax.rem(pz + d + NZ, NZ)

    first, last = pz == 0, pz == NZ - 1
    right = (g, jnp.where((pc == 1) & last, turn_x(1), px), jnp.where(pc == 1, turn_z(1), pz), 1 - pc)
    left = (g, jnp.where((pc == 0) & first, turn_x(-1), px), jnp.where(pc == 0, turn_z(-1), pz), 1 - pc)
    far = tuple(jnp.where(pc == 1, a, b) for a, b in zip(right, left))
    partner = (g, px, pz, 1 - pc)
    is_root, is_caster, is_end = first & (pc == 1), first & (pc == 0), last & (pc == 1)
    by_way = (g, jnp.where(is_caster, turn_x(-1), left[1]), jnp.where(is_caster, 0, left[2]), left[3])
    way_slot = jnp.where(is_caster, 2, 1)

    loads = [
        pltpu.make_async_copy(a, b, in_sem.at[i])
        for i, (a, b) in enumerate(((x_h, x), (tiles_h, tiles), (mass_h, mass), (src_h, src), (cols_h, cols)))
    ]
    for load in loads:
        load.start()

    def greet(x_at, z_at, c_at):
        pl.semaphore_signal(bar, inc=1, device_id=(g, x_at, z_at, c_at), device_id_type=MESH)

    greet(*partner[1:])

    @pl.when(jnp.logical_not(is_end))
    def _():
        greet(*far[1:])

    @pl.when(first)
    def _():
        for d in range(nx):
            for c in range(2):
                greet(turn_x(d), NZ - 1, c)
                if d > 0:
                    greet(turn_x(d), 0, c)

    @pl.when(is_root)
    def _():
        def greet_line(k, carry):
            greet(px, NZ - 1 - k, 0)
            greet(px, NZ - 1 - k, 1)
            return carry

        lax.fori_loop(1, NZ - 1, greet_line, 0)

    mates = 2 * nx - 1
    pl.semaphore_wait(
        bar, jnp.where(first, mates + jnp.where(is_root, 1, 0), jnp.where(last, 2 + 2 * nx, 3))
    )

    def send(src, dst, ss, rs, to):
        pltpu.make_async_remote_copy(src, dst, ss, rs, device_id=to, device_id_type=MESH).start()

    def landed(ref, sem):
        pltpu.make_async_copy(ref, ref, sem).wait()

    @pl.when(is_end)
    def _():
        pl.semaphore_signal(up_sem, inc=1, device_id=(g, px, 0, 1), device_id_type=MESH)

    loads[0].wait()
    send(x.at[pl.ds(0, tile)], halo_x.at[way_slot], large, x_rs.at[way_slot], by_way)
    send(x.at[pl.ds(tile, tile)], halo_x.at[0], large, x_rs.at[0], right)
    for load in loads[1:]:
        load.wait()

    position = (px * NZ + pz) * 2 + pc
    parts = []
    for b in range(2):
        here = position * 2 + b
        found = []
        for d in (-1, 0, 1):
            found.append(sum((cols[b, k] == here + d).astype(F32) * tiles[3 * b + k] for k in range(3)))
        parts.append(found)
    (t0l, t00, t01), (t10, t11, t1r) = parts
    eye = lax.broadcasted_iota(jnp.int32, (tile, tile), 0) == lax.broadcasted_iota(jnp.int32, (tile, tile), 1)
    ones = jnp.ones((tile, tile), BF16)
    diag = []
    for b in range(2):
        row = mass[pl.ds(b * tile, tile)].reshape(1, tile)
        rest = jnp.where(eye, row, 0.0) + (parts[b][0] + parts[b][1] + parts[b][2])
        high = rest.astype(BF16)
        rest = rest - high.astype(F32)
        mid = rest.astype(BF16)
        low = (rest - mid.astype(F32)).astype(BF16)
        diag.append(sum(jnp.dot(part, ones, preferred_element_type=F32) for part in (low, mid, high)))
    diag_last = diag[1]
    diag = jnp.concatenate(diag, axis=0)
    inner = halves(jnp.concatenate([jnp.concatenate([t00, t01], axis=1), jnp.concatenate([t10, t11], axis=1)], axis=0))
    to_left, to_right = halves(t0l), halves(t1r)

    x_pair = pair(x[...])
    ids = lax.broadcasted_iota(jnp.int32, (2 * tile, src.shape[0]), 0) + position * 2 * tile
    rhs = (ids == src[...].reshape(1, -1)).astype(F32)
    s = rhs - diag * x[...] + product(*inner, x_pair)
    s_buf[0] = s[:tile]
    s_buf[1] = s[tile:]
    m_buf[...] = jnp.where(eye, diag_last, 0.0) - t11
    from_left, from_right = halves(t0l.T), halves(t1r.T)
    send(s_buf.at[0], halo_s.at[way_slot], large, s_rs.at[way_slot], by_way)
    send(s_buf.at[1], halo_s.at[0], large, s_rs.at[0], right)
    to_chip = [
        pltpu.make_async_remote_copy(m_buf, halo_m, large, mw_rs, device_id=right, device_id_type=MESH),
        pltpu.make_async_remote_copy(q_buf, halo_q, large, qz_rs, device_id=right, device_id_type=MESH),
    ]

    passed = [
        pltpu.make_async_remote_copy(
            ref.at[2], ref.at[1], passing, rs.at[1], device_id=(g, px, NZ - 1, 1), device_id_type=MESH
        )
        for ref, rs in ((halo_x, x_rs), (halo_s, s_rs))
    ]

    @pl.when(is_root)
    def _():
        landed(halo_x.at[2], x_rs.at[2])
        landed(halo_s.at[2], s_rs.at[2])
        pl.semaphore_wait(up_sem, 1)
        for copy in passed:
            copy.start()

    @pl.when(pc == 1)
    def _():
        to_chip[0].start()
        landed(halo_x.at[0], x_rs.at[0])
        behind = s[:tile] + product(*to_left, pair(halo_x[0]))
        whole = jnp.concatenate([behind, s[tile:]], axis=0)
        q_buf[...] = diag_last * s[tile:] - product(inner[0][tile:], inner[1][tile:], pair(whole))
        to_chip[1].start()

    on_left = product(*from_left, x_pair[:tile])
    on_right = product(*from_right, x_pair[tile:])

    @pl.when(pc == 0)
    def _():
        landed(halo_x.at[0], x_rs.at[0])

    landed(halo_x.at[1], x_rs.at[1])
    r = s + jnp.concatenate([product(*to_left, pair(halo_x[0])), product(*to_right, pair(halo_x[1]))], axis=0)
    r_pair = pair(r)
    near_r = diag * r - product(*inner, r_pair)
    back_r = product(*from_left, r_pair[:tile])
    landed(halo_s.at[0], s_rs.at[0])
    landed(halo_s.at[1], s_rs.at[1])
    next_r = [halo_s[0] + on_left, halo_s[1] + on_right]
    w = near_r - jnp.concatenate([product(*to_left, pair(next_r[0])), product(*to_right, pair(next_r[1]))], axis=0)
    to_core = pltpu.make_async_remote_copy(
        w_buf, halo_w, large, mw_rs, device_id=partner, device_id_type=MESH
    )

    @pl.when(pc == 0)
    def _():
        w_buf[...] = w[tile:]
        to_core.start()


    w_pair = pair(w)
    sq, cross = rows_sum(r * r), rows_sum(r * w)
    ceiling = 2.0 * jnp.max(diag)
    about = jnp.where(sq > 0, jnp.clip(cross / sq, 0.0, ceiling), 0.0)
    u = w - about * r
    rss = rows_sum(u * u)
    near_u = diag * w - product(*inner, w_pair) - about * near_r
    back_u = product(*from_left, w_pair[:tile]) - about * back_r
    quad, lin, curv = rows_sum(u * near_u), 2.0 * rows_sum(r * near_u), rows_sum(r * near_r)

    @pl.when(pc == 0)
    def _():
        landed(halo_m, mw_rs)
        across_m = product(*halves(halo_m[...]), pair(on_left)) - back_r
        landed(halo_q, qz_rs)
        halo_w[...] = halo_q[...] + across_m

    @pl.when(pc == 1)
    def _():
        landed(halo_w, mw_rs)

    next_u = halo_w[...] - about * next_r[0]
    quad -= 2.0 * rows_sum(back_u * next_u)
    lin -= 2.0 * rows_sum(back_u * next_r[0] + back_r * next_u)
    curv -= 2.0 * rows_sum(back_r * next_r[0])
    blank = jnp.zeros((1, sq.shape[1]), F32)
    mine = jnp.concatenate([sq, cross, about, rss, quad, lin, curv, blank], axis=0)
    own[...] = mine

    edge_plane = first | last
    slot = jnp.where(edge_plane, nx + jnp.where(first, 2 * nx, 0) + px * 2 + pc, 0)
    rank = jnp.where(edge_plane, 0, (pz - 1) * 2 + pc)
    others = [(d, c) for d in (2, 1, nx - 1, 0) for c in range(2) if (d, c) != (0, 0)]

    def share(src, at, targets):
        return [
            pltpu.make_async_remote_copy(
                src, late.at[at], small, l_rs, device_id=(g, turn_x(d), 0, lax.rem(pc + c, 2)), device_id_type=MESH
            )
            for d, c in targets
        ]

    mine_out, line_out = share(own, slot, others), share(line, px, others)
    (mine_down,) = share(own, slot, [(0, 0)])
    mine_to_root = pltpu.make_async_remote_copy(
        own, ranks.at[rank], small, qz_rs, device_id=(g, px, 0, 1), device_id_type=MESH
    )

    @pl.when(edge_plane)
    def _():
        for copy in mine_out:
            copy.start()

    @pl.when(last)
    def _():
        mine_down.start()

    @pl.when(jnp.logical_not(edge_plane))
    def _():
        mine_to_root.start()

    count = 5 * nx

    @pl.when(is_root)
    def _():
        inner_planes = ranks.at[pl.ds(0, 2 * NZ - 4)]
        landed(inner_planes, qz_rs)
        joined = jnp.concatenate([*merged(inner_planes), blank], axis=0)
        line[...] = joined
        for copy in line_out:
            copy.start()
        late[px] = joined
        late[slot] = mine
        landed(late.at[pl.ds(0, count - 2)], l_rs)

    @pl.when(is_caster)
    def _():
        late[slot] = mine
        landed(late.at[pl.ds(0, count - 1)], l_rs)

    def to_chip_at(k):
        return [
            pltpu.make_async_remote_copy(total, total, small, l_rs, device_id=(g, px, k, c), device_id_type=MESH)
            for c in (1, 0)
        ]

    @pl.when(first)
    def _():
        sq, cross, _, rss, quad, _, _ = merged(late)
        step = sq / cross
        after = step * step * rss
        ratio = after / sq
        step_next = after / (step * step * quad - ratio * after / step)
        total[...] = jnp.concatenate(
            [step + step_next * (1.0 + ratio), -(step_next * step), jnp.zeros((6, sq.shape[1]), F32)], axis=0
        )

    @pl.when(jnp.logical_not(first))
    def _():
        landed(total, l_rs)

    is_second = last & (pc == 0)

    @pl.when(is_caster)
    def _():
        for k in (*range(1, NEAR + 1), NZ - 1):
            for copy in to_chip_at(k):
                copy.start()

    @pl.when(is_second)
    def _():
        def step(k, carry):
            for copy in to_chip_at(k):
                copy.start()
            return carry

        lax.fori_loop(NEAR + 1, NZ - 1, step, 0)

    out[...] = x[...] + total[0:1] * r + total[1:2] * w

    @pl.when(pc == 0)
    def _():
        landed(tiles.at[pl.ds(0, 5)], large)

    @pl.when(pc == 1)
    def _():
        landed(tiles, large)

    @pl.when(is_root)
    def _():
        landed(halo_x.at[pl.ds(0, 2)], passing)
        landed(ranks.at[pl.ds(0, 2 * mates)], small)

    @pl.when(is_caster)
    def _():
        landed(ranks.at[pl.ds(0, mates + 2 * (NEAR + 1))], small)

    @pl.when(is_second)
    def _():
        landed(ranks.at[pl.ds(0, mates + 1 + 2 * (NZ - 2 - NEAR))], small)

    @pl.when(is_end)
    def _():
        landed(ranks.at[pl.ds(0, mates + 1)], small)

    @pl.when(jnp.logical_not(edge_plane))
    def _():
        mine_to_root.wait_send()


def body(block_cols, step_tiles, mass, warm_start, source_ids):
    nx = lax.axis_size("patch_0")
    tile = step_tiles.shape[-1]
    rows, width = warm_start.shape
    edge, slots, square, sums = (2, tile, width), (3, tile, width), (tile, tile), (8, width)
    sem = pltpu.SemaphoreType.DMA
    return pl.pallas_call(
        functools.partial(kernel, nx, tile),
        out_shape=pltpu.VMEM((rows, width), F32),
        in_specs=[ANY] * 5,
        out_specs=pl.BlockSpec(memory_space=pltpu.VMEM),
        scratch_shapes=[
            pltpu.SMEM(block_cols.shape, jnp.int32),
            pltpu.VMEM((6, tile, tile), F32),
            pltpu.VMEM(mass.shape, F32),
            pltpu.VMEM((rows, width), F32),
            pltpu.VMEM(source_ids.shape, jnp.int32),
            pltpu.VMEM(slots, F32), pltpu.VMEM(slots, F32), pltpu.VMEM(edge[1:], F32),
            pltpu.VMEM(square, F32), pltpu.VMEM(edge[1:], F32),
            pltpu.VMEM(edge, F32), pltpu.VMEM(edge[1:], F32),
            pltpu.VMEM(square, F32), pltpu.VMEM(edge[1:], F32),
            pltpu.VMEM(sums, F32),
            pltpu.VMEM((2 * NZ - 4, *sums), F32),
            pltpu.VMEM(sums, F32),
            pltpu.VMEM((5 * nx, *sums), F32),
            pltpu.VMEM(sums, F32),
            sem((5,)),
            sem((3,)), sem((3,)),
            sem, sem,
            pltpu.SemaphoreType.REGULAR,
            sem,
        ],
        compiler_params=pltpu.CompilerParams(collective_id=0, has_side_effects=True),
        name="heat",
    )(block_cols, step_tiles.reshape(6, tile, tile), mass, warm_start, source_ids)


def solution(mesh):
    split = Mesh(
        mesh.devices.reshape(mesh.shape["groups"], mesh.shape["patch"] // NZ, NZ, mesh.shape["sub"]), AXES
    )
    placed = (P(AXES, None), P(AXES, None, None, None), P(AXES), P(AXES, None), P("groups"))
    return jax.shard_map(body, mesh=split, in_specs=placed, out_specs=P(AXES, None), check_vma=False)
```

```python
import functools

import jax
import jax.numpy as jnp
from jax import lax
from jax.experimental import pallas as pl
from jax.experimental.pallas import tpu as pltpu
from jax.sharding import Mesh
from jax.sharding import PartitionSpec as P

NZ = 32
NEAR = 4
AXES = ("groups", "patch_0", "patch_1", "sub")
MESH = pl.DeviceIdType.MESH
F32, BF16 = jnp.float32, jnp.bfloat16
ANY = pl.BlockSpec(memory_space=pl.ANY)


def halves(value):
    high = value.astype(BF16)
    return high, (value - high.astype(F32)).astype(BF16)


def pair(value):
    return jnp.concatenate(halves(value), axis=1)


def product(high, low, packed):
    n = packed.shape[1] // 2
    both = jnp.dot(high, packed, preferred_element_type=F32) + jnp.dot(low, packed, preferred_element_type=F32)
    return both[:, :n] + both[:, n:]


def rows_sum(value):
    return jnp.sum(value, axis=0, keepdims=True)


def merged(buf):
    sq, cross, about, rss, quad, lin, curv = (buf[:, k, :] for k in range(7))
    sq_all, cross_all = rows_sum(sq), rows_sum(cross)
    centre = jnp.where(sq_all > 0, cross_all / sq_all, 0.0)
    off = about - centre
    first = cross - about * sq
    rss_all = rows_sum(rss + off * (2.0 * first + off * sq))
    quad_all = rows_sum(quad + off * (lin + off * curv))
    lin_all = rows_sum(lin + 2.0 * off * curv)
    return sq_all, cross_all, centre, rss_all, quad_all, lin_all, rows_sum(curv)


def kernel(
    nx, tile,
    cols_h, tiles_h, mass_h, x_h, src_h,
    out,
    cols, tiles, mass, x, src,
    halo_x, halo_s, halo_w, halo_m, halo_q, s_buf, w_buf, m_buf, q_buf, own, ranks, line, late, total,
    in_sem, x_rs, s_rs, mw_rs, qz_rs, up_sem, l_rs,
):
    large, small, passing = in_sem.at[0], in_sem.at[1], in_sem.at[2]
    g, px, pz, pc = (lax.axis_index(name) for name in AXES)
    bar = pltpu.get_barrier_semaphore()

    def turn_x(d):
        return lax.rem(px + d + nx, nx)

    def turn_z(d):
        return lax.rem(pz + d + NZ, NZ)

    first, last = pz == 0, pz == NZ - 1
    right = (g, jnp.where((pc == 1) & last, turn_x(1), px), jnp.where(pc == 1, turn_z(1), pz), 1 - pc)
    left = (g, jnp.where((pc == 0) & first, turn_x(-1), px), jnp.where(pc == 0, turn_z(-1), pz), 1 - pc)
    far = tuple(jnp.where(pc == 1, a, b) for a, b in zip(right, left))
    partner = (g, px, pz, 1 - pc)
    is_root, is_caster, is_end = first & (pc == 1), first & (pc == 0), last & (pc == 1)
    by_way = (g, jnp.where(is_caster, turn_x(-1), left[1]), jnp.where(is_caster, 0, left[2]), left[3])
    way_slot = jnp.where(is_caster, 2, 1)

    loads = [
        pltpu.make_async_copy(a, b, in_sem.at[i])
        for i, (a, b) in enumerate(((x_h, x), (tiles_h, tiles), (mass_h, mass), (src_h, src), (cols_h, cols)))
    ]
    for load in loads:
        load.start()

    def greet(x_at, z_at, c_at):
        pl.semaphore_signal(bar, inc=1, device_id=(g, x_at, z_at, c_at), device_id_type=MESH)

    greet(*partner[1:])

    @pl.when(jnp.logical_not(is_end))
    def _():
        greet(*far[1:])

    @pl.when(first)
    def _():
        for d in range(nx):
            for c in range(2):
                greet(turn_x(d), NZ - 1, c)
                if d > 0:
                    greet(turn_x(d), 0, c)

    @pl.when(is_root)
    def _():
        def greet_line(k, carry):
            greet(px, NZ - 1 - k, 0)
            greet(px, NZ - 1 - k, 1)
            return carry

        lax.fori_loop(1, NZ - 1, greet_line, 0)

    mates = 2 * nx - 1
    pl.semaphore_wait(
        bar, jnp.where(first, mates + jnp.where(is_root, 1, 0), jnp.where(last, 2 + 2 * nx, 3))
    )

    def send(src, dst, ss, rs, to):
        pltpu.make_async_remote_copy(src, dst, ss, rs, device_id=to, device_id_type=MESH).start()

    def landed(ref, sem):
        pltpu.make_async_copy(ref, ref, sem).wait()

    @pl.when(is_end)
    def _():
        pl.semaphore_signal(up_sem, inc=1, device_id=(g, px, 0, 1), device_id_type=MESH)

    loads[0].wait()
    send(x.at[pl.ds(0, tile)], halo_x.at[way_slot], large, x_rs.at[way_slot], by_way)
    send(x.at[pl.ds(tile, tile)], halo_x.at[0], large, x_rs.at[0], right)
    for load in loads[1:]:
        load.wait()

    position = (px * NZ + pz) * 2 + pc
    parts = []
    for b in range(2):
        here = position * 2 + b
        found = []
        for d in (-1, 0, 1):
            found.append(sum((cols[b, k] == here + d).astype(F32) * tiles[3 * b + k] for k in range(3)))
        parts.append(found)
    (t0l, t00, t01), (t10, t11, t1r) = parts
    eye = lax.broadcasted_iota(jnp.int32, (tile, tile), 0) == lax.broadcasted_iota(jnp.int32, (tile, tile), 1)
    ones = jnp.ones((tile, tile), BF16)
    diag = []
    for b in range(2):
        row = mass[pl.ds(b * tile, tile)].reshape(1, tile)
        rest = jnp.where(eye, row, 0.0) + (parts[b][0] + parts[b][1] + parts[b][2])
        high = rest.astype(BF16)
        rest = rest - high.astype(F32)
        mid = rest.astype(BF16)
        low = (rest - mid.astype(F32)).astype(BF16)
        diag.append(sum(jnp.dot(part, ones, preferred_element_type=F32) for part in (low, mid, high)))
    diag_last = diag[1]
    diag = jnp.concatenate(diag, axis=0)
    inner = halves(jnp.concatenate([jnp.concatenate([t00, t01], axis=1), jnp.concatenate([t10, t11], axis=1)], axis=0))
    to_left, to_right = halves(t0l), halves(t1r)

    x_pair = pair(x[...])
    ids = lax.broadcasted_iota(jnp.int32, (2 * tile, src.shape[0]), 0) + position * 2 * tile
    rhs = (ids == src[...].reshape(1, -1)).astype(F32)
    s = rhs - diag * x[...] + product(*inner, x_pair)
    s_buf[0] = s[:tile]
    s_buf[1] = s[tile:]
    m_buf[...] = jnp.where(eye, diag_last, 0.0) - t11
    from_left, from_right = halves(t0l.T), halves(t1r.T)
    send(s_buf.at[0], halo_s.at[way_slot], large, s_rs.at[way_slot], by_way)
    send(s_buf.at[1], halo_s.at[0], large, s_rs.at[0], right)
    to_chip = [
        pltpu.make_async_remote_copy(m_buf, halo_m, large, mw_rs, device_id=right, device_id_type=MESH),
        pltpu.make_async_remote_copy(q_buf, halo_q, large, qz_rs, device_id=right, device_id_type=MESH),
    ]

    passed = [
        pltpu.make_async_remote_copy(
            ref.at[2], ref.at[1], passing, rs.at[1], device_id=(g, px, NZ - 1, 1), device_id_type=MESH
        )
        for ref, rs in ((halo_x, x_rs), (halo_s, s_rs))
    ]

    @pl.when(is_root)
    def _():
        landed(halo_x.at[2], x_rs.at[2])
        landed(halo_s.at[2], s_rs.at[2])
        pl.semaphore_wait(up_sem, 1)
        for copy in passed:
            copy.start()

    @pl.when(pc == 1)
    def _():
        to_chip[0].start()
        landed(halo_x.at[0], x_rs.at[0])
        behind = s[:tile] + product(*to_left, pair(halo_x[0]))
        whole = jnp.concatenate([behind, s[tile:]], axis=0)
        q_buf[...] = diag_last * s[tile:] - product(inner[0][tile:], inner[1][tile:], pair(whole))
        to_chip[1].start()

    on_left = product(*from_left, x_pair[:tile])
    on_right = product(*from_right, x_pair[tile:])

    @pl.when(pc == 0)
    def _():
        landed(halo_x.at[0], x_rs.at[0])

    landed(halo_x.at[1], x_rs.at[1])
    r = s + jnp.concatenate([product(*to_left, pair(halo_x[0])), product(*to_right, pair(halo_x[1]))], axis=0)
    r_pair = pair(r)
    near_r = diag * r - product(*inner, r_pair)
    back_r = product(*from_left, r_pair[:tile])
    landed(halo_s.at[0], s_rs.at[0])
    landed(halo_s.at[1], s_rs.at[1])
    next_r = [halo_s[0] + on_left, halo_s[1] + on_right]
    w = near_r - jnp.concatenate([product(*to_left, pair(next_r[0])), product(*to_right, pair(next_r[1]))], axis=0)
    to_core = pltpu.make_async_remote_copy(
        w_buf, halo_w, large, mw_rs, device_id=partner, device_id_type=MESH
    )

    @pl.when(pc == 0)
    def _():
        w_buf[...] = w[tile:]
        to_core.start()


    w_pair = pair(w)
    sq, cross = rows_sum(r * r), rows_sum(r * w)
    ceiling = 2.0 * jnp.max(diag)
    about = jnp.where(sq > 0, jnp.clip(cross / sq, 0.0, ceiling), 0.0)
    u = w - about * r
    rss = rows_sum(u * u)
    near_u = diag * w - product(*inner, w_pair) - about * near_r
    back_u = product(*from_left, w_pair[:tile]) - about * back_r
    quad, lin, curv = rows_sum(u * near_u), 2.0 * rows_sum(r * near_u), rows_sum(r * near_r)

    @pl.when(pc == 0)
    def _():
        landed(halo_m, mw_rs)
        across_m = product(*halves(halo_m[...]), pair(on_left)) - back_r
        landed(halo_q, qz_rs)
        halo_w[...] = halo_q[...] + across_m

    @pl.when(pc == 1)
    def _():
        landed(halo_w, mw_rs)

    next_u = halo_w[...] - about * next_r[0]
    quad -= 2.0 * rows_sum(back_u * next_u)
    lin -= 2.0 * rows_sum(back_u * next_r[0] + back_r * next_u)
    curv -= 2.0 * rows_sum(back_r * next_r[0])
    blank = jnp.zeros((1, sq.shape[1]), F32)
    mine = jnp.concatenate([sq, cross, about, rss, quad, lin, curv, blank], axis=0)
    own[...] = mine

    edge_plane = first | last
    slot = jnp.where(edge_plane, nx + jnp.where(first, 2 * nx, 0) + px * 2 + pc, 0)
    rank = jnp.where(edge_plane, 0, (pz - 1) * 2 + pc)
    others = [(d, c) for d in (2, 1, nx - 1, 0) for c in range(2) if (d, c) != (0, 0)]

    def share(src, at, targets):
        return [
            pltpu.make_async_remote_copy(
                src, late.at[at], small, l_rs, device_id=(g, turn_x(d), 0, lax.rem(pc + c, 2)), device_id_type=MESH
            )
            for d, c in targets
        ]

    mine_out, line_out = share(own, slot, others), share(line, px, others)
    (mine_down,) = share(own, slot, [(0, 0)])
    mine_to_root = pltpu.make_async_remote_copy(
        own, ranks.at[rank], small, qz_rs, device_id=(g, px, 0, 1), device_id_type=MESH
    )

    @pl.when(edge_plane)
    def _():
        for copy in mine_out:
            copy.start()

    @pl.when(last)
    def _():
        mine_down.start()

    @pl.when(jnp.logical_not(edge_plane))
    def _():
        mine_to_root.start()

    count = 5 * nx

    @pl.when(is_root)
    def _():
        inner_planes = ranks.at[pl.ds(0, 2 * NZ - 4)]
        landed(inner_planes, qz_rs)
        joined = jnp.concatenate([*merged(inner_planes), blank], axis=0)
        line[...] = joined
        for copy in line_out:
            copy.start()
        late[px] = joined
        late[slot] = mine
        landed(late.at[pl.ds(0, count - 2)], l_rs)

    @pl.when(is_caster)
    def _():
        late[slot] = mine
        landed(late.at[pl.ds(0, count - 1)], l_rs)

    def to_chip_at(k, x_at=px):
        return [
            pltpu.make_async_remote_copy(total, total, small, l_rs, device_id=(g, x_at, k, c), device_id_type=MESH)
            for c in (1, 0)
        ]

    @pl.when(first)
    def _():
        sq, cross, _, rss, quad, _, _ = merged(late)
        step = sq / cross
        after = step * step * rss
        ratio = after / sq
        step_next = after / (step * step * quad - ratio * after / step)
        total[...] = jnp.concatenate(
            [step + step_next * (1.0 + ratio), -(step_next * step), jnp.zeros((6, sq.shape[1]), F32)], axis=0
        )

    @pl.when(jnp.logical_not(first))
    def _():
        landed(total, l_rs)

    is_second = last & (pc == 0)
    serves, is_server = is_caster & (px > 0), is_root & (px == nx - 1)

    @pl.when(serves | is_server)
    def _():
        for k in (*range(1, NEAR + 1), NZ - 1):
            for copy in to_chip_at(k, jnp.where(is_server, 0, px)):
                copy.start()

    @pl.when(is_second)
    def _():
        def step(k, carry):
            for copy in to_chip_at(k):
                copy.start()
            return carry

        lax.fori_loop(NEAR + 1, NZ - 1, step, 0)

    out[...] = x[...] + total[0:1] * r + total[1:2] * w

    @pl.when(pc == 0)
    def _():
        landed(tiles.at[pl.ds(0, 5)], large)

    @pl.when(pc == 1)
    def _():
        landed(tiles, large)

    @pl.when(is_root)
    def _():
        landed(halo_x.at[pl.ds(0, 2)], passing)

    @pl.when(is_root & (px < nx - 1))
    def _():
        landed(ranks.at[pl.ds(0, 2 * mates)], small)

    @pl.when(is_server)
    def _():
        landed(ranks.at[pl.ds(0, 2 * mates + 2 * (NEAR + 1))], small)

    @pl.when(is_caster & (px == 0))
    def _():
        landed(ranks.at[pl.ds(0, mates)], small)

    @pl.when(serves)
    def _():
        landed(ranks.at[pl.ds(0, mates + 2 * (NEAR + 1))], small)

    @pl.when(is_second)
    def _():
        landed(ranks.at[pl.ds(0, mates + 1 + 2 * (NZ - 2 - NEAR))], small)

    @pl.when(is_end)
    def _():
        landed(ranks.at[pl.ds(0, mates + 1)], small)

    @pl.when(jnp.logical_not(edge_plane))
    def _():
        mine_to_root.wait_send()


def body(block_cols, step_tiles, mass, warm_start, source_ids):
    nx = lax.axis_size("patch_0")
    tile = step_tiles.shape[-1]
    rows, width = warm_start.shape
    edge, slots, square, sums = (2, tile, width), (3, tile, width), (tile, tile), (8, width)
    sem = pltpu.SemaphoreType.DMA
    return pl.pallas_call(
        functools.partial(kernel, nx, tile),
        out_shape=pltpu.VMEM((rows, width), F32),
        in_specs=[ANY] * 5,
        out_specs=pl.BlockSpec(memory_space=pltpu.VMEM),
        scratch_shapes=[
            pltpu.SMEM(block_cols.shape, jnp.int32),
            pltpu.VMEM((6, tile, tile), F32),
            pltpu.VMEM(mass.shape, F32),
            pltpu.VMEM((rows, width), F32),
            pltpu.VMEM(source_ids.shape, jnp.int32),
            pltpu.VMEM(slots, F32), pltpu.VMEM(slots, F32), pltpu.VMEM(edge[1:], F32),
            pltpu.VMEM(square, F32), pltpu.VMEM(edge[1:], F32),
            pltpu.VMEM(edge, F32), pltpu.VMEM(edge[1:], F32),
            pltpu.VMEM(square, F32), pltpu.VMEM(edge[1:], F32),
            pltpu.VMEM(sums, F32),
            pltpu.VMEM((2 * NZ - 4, *sums), F32),
            pltpu.VMEM(sums, F32),
            pltpu.VMEM((5 * nx, *sums), F32),
            pltpu.VMEM(sums, F32),
            sem((5,)),
            sem((3,)), sem((3,)),
            sem, sem,
            pltpu.SemaphoreType.REGULAR,
            sem,
        ],
        compiler_params=pltpu.CompilerParams(collective_id=0, has_side_effects=True),
        name="heat",
    )(block_cols, step_tiles.reshape(6, tile, tile), mass, warm_start, source_ids)


def solution(mesh):
    split = Mesh(
        mesh.devices.reshape(mesh.shape["groups"], mesh.shape["patch"] // NZ, NZ, mesh.shape["sub"]), AXES
    )
    placed = (P(AXES, None), P(AXES, None, None, None), P(AXES), P(AXES, None), P("groups"))
    return jax.shard_map(body, mesh=split, in_specs=placed, out_specs=P(AXES, None), check_vma=False)
```

```python
import functools

import jax
import jax.numpy as jnp
from jax import lax
from jax.experimental import pallas as pl
from jax.experimental.pallas import tpu as pltpu
from jax.sharding import Mesh
from jax.sharding import PartitionSpec as P

NZ = 32
NEAR = 4
AXES = ("groups", "patch_0", "patch_1", "sub")
MESH = pl.DeviceIdType.MESH
F32, BF16 = jnp.float32, jnp.bfloat16
ANY = pl.BlockSpec(memory_space=pl.ANY)


def halves(value):
    high = value.astype(BF16)
    return high, (value - high.astype(F32)).astype(BF16)


def pair(value):
    return jnp.concatenate(halves(value), axis=1)


def product(high, low, packed):
    n = packed.shape[1] // 2
    both = jnp.dot(high, packed, preferred_element_type=F32)
    return both[:, :n] + (both[:, n:] + jnp.dot(low, packed[:, :n], preferred_element_type=F32))


def rows_sum(value):
    return jnp.sum(value, axis=0, keepdims=True)


def merged(buf):
    sq, cross, about, rss, quad, lin, curv = (buf[:, k, :] for k in range(7))
    sq_all, cross_all = rows_sum(sq), rows_sum(cross)
    centre = jnp.where(sq_all > 0, cross_all / sq_all, 0.0)
    off = about - centre
    first = cross - about * sq
    rss_all = rows_sum(rss + off * (2.0 * first + off * sq))
    quad_all = rows_sum(quad + off * (lin + off * curv))
    lin_all = rows_sum(lin + 2.0 * off * curv)
    return sq_all, cross_all, centre, rss_all, quad_all, lin_all, rows_sum(curv)


def kernel(
    nx, tile,
    cols_h, tiles_h, mass_h, x_h, src_h,
    out,
    cols, tiles, mass, x, src,
    halo_x, halo_s, halo_c, halo_m, halo_q, s_buf, c_buf, m_buf, q_buf, own, ranks, line, late, total,
    in_sem, x_rs, s_rs, m_rs, q_rs, y_rs, c_rs, z_rs, up_sem, l_rs,
):
    large, small, passing = in_sem.at[0], in_sem.at[1], in_sem.at[2]
    g, px, pz, pc = (lax.axis_index(name) for name in AXES)
    bar = pltpu.get_barrier_semaphore()

    def turn_x(d):
        return lax.rem(px + d + nx, nx)

    def turn_z(d):
        return lax.rem(pz + d + NZ, NZ)

    first, last = pz == 0, pz == NZ - 1
    right = (g, jnp.where((pc == 1) & last, turn_x(1), px), jnp.where(pc == 1, turn_z(1), pz), 1 - pc)
    left = (g, jnp.where((pc == 0) & first, turn_x(-1), px), jnp.where(pc == 0, turn_z(-1), pz), 1 - pc)
    far = tuple(jnp.where(pc == 1, a, b) for a, b in zip(right, left))
    partner = (g, px, pz, 1 - pc)
    is_root, is_caster, is_end = first & (pc == 1), first & (pc == 0), last & (pc == 1)
    by_way = (g, jnp.where(is_caster, turn_x(-1), left[1]), jnp.where(is_caster, 0, left[2]), left[3])
    way_slot = jnp.where(is_caster, 2, 1)

    loads = [
        pltpu.make_async_copy(a, b, in_sem.at[i])
        for i, (a, b) in enumerate(((x_h, x), (tiles_h, tiles), (mass_h, mass), (src_h, src), (cols_h, cols)))
    ]
    for load in loads:
        load.start()

    def greet(x_at, z_at, c_at):
        pl.semaphore_signal(bar, inc=1, device_id=(g, x_at, z_at, c_at), device_id_type=MESH)

    greet(*partner[1:])

    @pl.when(jnp.logical_not(is_end))
    def _():
        greet(*far[1:])

    @pl.when((pc == 1) & jnp.logical_not(first))
    def _():
        greet(px, pz - 1, 1)

    @pl.when(first)
    def _():
        for d in range(nx):
            for c in range(2):
                greet(turn_x(d), NZ - 1, c)
                if d > 0:
                    greet(turn_x(d), 0, c)

    @pl.when(is_root)
    def _():
        def greet_line(k, carry):
            greet(px, NZ - 1 - k, 0)
            greet(px, NZ - 1 - k, 1)
            return carry

        lax.fori_loop(1, NZ - 1, greet_line, 0)

    mates = 2 * nx - 1
    pl.semaphore_wait(
        bar, jnp.where(first, mates + 2 * pc, jnp.where(last, 2 + 2 * nx, 3 + pc))
    )

    def send(src, dst, ss, rs, to):
        pltpu.make_async_remote_copy(src, dst, ss, rs, device_id=to, device_id_type=MESH).start()

    def landed(ref, sem):
        pltpu.make_async_copy(ref, ref, sem).wait()

    @pl.when(is_end)
    def _():
        pl.semaphore_signal(up_sem, inc=1, device_id=(g, px, 0, 1), device_id_type=MESH)

    loads[0].wait()
    send(x.at[pl.ds(0, tile)], halo_x.at[way_slot], large, x_rs.at[way_slot], by_way)
    send(x.at[pl.ds(tile, tile)], halo_x.at[0], large, x_rs.at[0], right)
    for load in loads[1:]:
        load.wait()

    position = (px * NZ + pz) * 2 + pc
    parts = []
    for b in range(2):
        here = position * 2 + b
        found = []
        for d in (-1, 0, 1):
            found.append(sum((cols[b, k] == here + d).astype(F32) * tiles[3 * b + k] for k in range(3)))
        parts.append(found)
    (t0l, t00, t01), (t10, t11, t1r) = parts
    eye = lax.broadcasted_iota(jnp.int32, (tile, tile), 0) == lax.broadcasted_iota(jnp.int32, (tile, tile), 1)
    ones = jnp.ones((tile, tile), BF16)
    diag = []
    for b in range(2):
        row = mass[pl.ds(b * tile, tile)].reshape(1, tile)
        rest = jnp.where(eye, row, 0.0) + (parts[b][0] + parts[b][1] + parts[b][2])
        high = rest.astype(BF16)
        rest = rest - high.astype(F32)
        mid = rest.astype(BF16)
        low = (rest - mid.astype(F32)).astype(BF16)
        diag.append(sum(jnp.dot(part, ones, preferred_element_type=F32) for part in (low, mid, high)))
    diag_last = diag[1]
    diag = jnp.concatenate(diag, axis=0)
    inner = halves(jnp.concatenate([jnp.concatenate([t00, t01], axis=1), jnp.concatenate([t10, t11], axis=1)], axis=0))
    to_left, to_right = halves(t0l), halves(t1r)

    ceiling = 2.0 * jnp.max(diag, axis=0, keepdims=True)
    x_pair = pair(x[...])
    ids = lax.broadcasted_iota(jnp.int32, (2 * tile, src.shape[0]), 0) + position * 2 * tile
    rhs = (ids == src[...].reshape(1, -1)).astype(F32)
    s = rhs - diag * x[...] + product(*inner, x_pair)
    s_buf[0] = s[:tile]
    s_buf[1] = s[tile:]
    m_buf[...] = jnp.where(eye, diag_last, 0.0) - t11
    from_left, from_right = halves(t0l.T), halves(t1r.T)
    send(s_buf.at[0], halo_s.at[way_slot], large, s_rs.at[way_slot], by_way)
    send(s_buf.at[1], halo_s.at[0], large, s_rs.at[0], right)
    to_chip = [
        pltpu.make_async_remote_copy(src, dst, large, rs, device_id=(*right[:3], 1), device_id_type=MESH)
        for src, dst, rs in ((m_buf, halo_m, m_rs), (q_buf, halo_q, q_rs))
    ]
    to_core = [
        pltpu.make_async_remote_copy(
            c_buf.at[i], halo_c.at[i], passing, y_rs if i == 4 else c_rs, device_id=partner, device_id_type=MESH
        )
        for i in range(5)
    ]

    passed = [
        pltpu.make_async_remote_copy(
            ref.at[2], ref.at[1], passing, rs.at[1], device_id=(g, px, NZ - 1, 1), device_id_type=MESH
        )
        for ref, rs in ((halo_x, x_rs), (halo_s, s_rs))
    ]

    @pl.when(is_root)
    def _():
        landed(halo_x.at[2], x_rs.at[2])
        landed(halo_s.at[2], s_rs.at[2])
        pl.semaphore_wait(up_sem, 1)
        for copy in passed:
            copy.start()

    @pl.when(pc == 1)
    def _():
        to_chip[0].start()
        landed(halo_x.at[0], x_rs.at[0])
        behind = s[:tile] + product(*to_left, pair(halo_x[0]))
        whole = jnp.concatenate([behind, s[tile:]], axis=0)
        q_buf[...] = diag_last * s[tile:] - product(inner[0][tile:], inner[1][tile:], pair(whole))
        to_chip[1].start()

    on_left = product(*from_left, x_pair[:tile])
    on_right = product(*from_right, x_pair[tile:])

    @pl.when(pc == 0)
    def _():
        c_buf[4] = on_left
        to_core[4].start()
        landed(halo_x.at[0], x_rs.at[0])

    landed(halo_x.at[1], x_rs.at[1])
    r = s + jnp.concatenate([product(*to_left, pair(halo_x[0])), product(*to_right, pair(halo_x[1]))], axis=0)
    r_pair = pair(r)
    near_r = diag * r - product(*inner, r_pair)
    back_r = product(*from_left, r_pair[:tile])
    landed(halo_s.at[0], s_rs.at[0])
    landed(halo_s.at[1], s_rs.at[1])
    next_r = [halo_s[0] + on_left, halo_s[1] + on_right]
    w = near_r - jnp.concatenate([product(*to_left, pair(next_r[0])), product(*to_right, pair(next_r[1]))], axis=0)

    @pl.when(pc == 0)
    def _():
        for i, value in enumerate((w[tile:], back_r, next_r[0])):
            c_buf[i] = value
            to_core[i].start()

    w_pair = pair(w)
    sq, cross = rows_sum(r * r), rows_sum(r * w)
    about = jnp.where(sq > 0, jnp.clip(cross / sq, 0.0, ceiling), 0.0)
    u = w - about * r
    rss = rows_sum(u * u)
    near_u = diag * w - product(*inner, w_pair) - about * near_r
    back_w = product(*from_left, w_pair[:tile])

    @pl.when(pc == 0)
    def _():
        c_buf[3] = back_w
        to_core[3].start()

    quad, lin, curv = rows_sum(u * near_u), 2.0 * rows_sum(r * near_u), rows_sum(r * near_r)

    own[...] = jnp.concatenate([sq, cross, about, rss, quad, lin, curv, jnp.zeros_like(sq)], axis=0)

    @pl.when(pc == 1)
    def _():
        landed(halo_c.at[4], y_rs)
        landed(halo_m, m_rs)
        across_m = product(*halves(halo_m[...]), pair(halo_c[4]))
        landed(halo_q, q_rs)
        landed(halo_c.at[pl.ds(0, 4)], c_rs)
        w_at, back_r_at, next_r_at, back_w_at = (halo_c[i] for i in range(4))
        quads, lins, curvs = quad, lin, curv
        for edge_w, edge_r, edge_back_w, edge_back_r in (
            (w_at, next_r[0], back_w, back_r),
            (halo_q[...] + across_m - back_r_at, next_r_at, back_w_at, back_r_at),
        ):
            edge_u, edge_back_u = edge_w - about * edge_r, edge_back_w - about * edge_back_r
            quads -= 2.0 * rows_sum(edge_back_u * edge_u)
            lins -= 2.0 * rows_sum(edge_back_u * edge_r + edge_back_r * edge_u)
            curvs -= 2.0 * rows_sum(edge_back_r * edge_r)
        own[pl.ds(4, 3), :] = jnp.concatenate([quads, lins, curvs], axis=0)

    blank = jnp.zeros((1, sq.shape[1]), F32)

    edge_plane = first | last
    slot = jnp.where(edge_plane, nx + jnp.where(first, 2 * nx, 0) + px * 2 + pc, 0)
    rank = jnp.where(edge_plane, 0, (pz - 1) * 2 + pc)
    others = [(d, c) for d in (2, 1, nx - 1, 0) for c in range(2) if (d, c) != (0, 0)]

    def share(src, at, targets):
        return [
            pltpu.make_async_remote_copy(
                src, late.at[at], small, l_rs, device_id=(g, turn_x(d), 0, lax.rem(pc + c, 2)), device_id_type=MESH
            )
            for d, c in targets
        ]

    mine_out, line_out = share(own, slot, others), share(line, px, others)
    (mine_down,) = share(own, slot, [(0, 0)])
    mine_to_root = pltpu.make_async_remote_copy(
        own, ranks.at[rank], small, z_rs, device_id=(g, px, 0, 1), device_id_type=MESH
    )

    @pl.when(edge_plane)
    def _():
        for copy in mine_out:
            copy.start()

    @pl.when(last)
    def _():
        mine_down.start()

    @pl.when(jnp.logical_not(edge_plane))
    def _():
        mine_to_root.start()

    count = 5 * nx

    @pl.when(is_root)
    def _():
        inner_planes = ranks.at[pl.ds(0, 2 * NZ - 4)]
        landed(inner_planes, z_rs)
        joined = jnp.concatenate([*merged(inner_planes), blank], axis=0)
        line[...] = joined
        for copy in line_out:
            copy.start()
        late[px] = joined
        late[slot] = own[...]
        landed(late.at[pl.ds(0, count - 2)], l_rs)

    @pl.when(is_caster)
    def _():
        late[slot] = own[...]
        landed(late.at[pl.ds(0, count - 1)], l_rs)

    def to_chip_at(k, x_at=px):
        return [
            pltpu.make_async_remote_copy(total, total, small, l_rs, device_id=(g, x_at, k, c), device_id_type=MESH)
            for c in (1, 0)
        ]

    @pl.when(first)
    def _():
        sq, cross, _, rss, quad, _, _ = merged(late)
        step = sq / cross
        after = step * step * rss
        ratio = after / sq
        step_next = after / (step * step * quad - ratio * after / step)
        total[...] = jnp.concatenate(
            [step + step_next * (1.0 + ratio), -(step_next * step), jnp.zeros((6, sq.shape[1]), F32)], axis=0
        )

    @pl.when(jnp.logical_not(first))
    def _():
        landed(total, l_rs)

    is_second = last & (pc == 0)
    serves, is_server = is_caster & (px > 0), is_root & (px == nx - 1)

    @pl.when(serves | is_server)
    def _():
        for k in (*range(1, NEAR + 1), NZ - 1):
            for copy in to_chip_at(k, jnp.where(is_server, 0, px)):
                copy.start()

    @pl.when(is_second)
    def _():
        def step(k, carry):
            for copy in to_chip_at(k):
                copy.start()
            return carry

        lax.fori_loop(NEAR + 1, NZ - 1, step, 0)

    out[...] = x[...] + total[0:1] * r + total[1:2] * w

    @pl.when(pc == 0)
    def _():
        landed(tiles.at[pl.ds(0, 4)], large)
        landed(tiles.at[pl.ds(0, 5)], passing)

    @pl.when(pc == 1)
    def _():
        landed(tiles, large)

    @pl.when(is_root)
    def _():
        landed(halo_x.at[pl.ds(0, 2)], passing)

    @pl.when(is_root & (px < nx - 1))
    def _():
        landed(ranks.at[pl.ds(0, 2 * mates)], small)

    @pl.when(is_server)
    def _():
        landed(ranks.at[pl.ds(0, 2 * mates + 2 * (NEAR + 1))], small)

    @pl.when(is_caster & (px == 0))
    def _():
        landed(ranks.at[pl.ds(0, mates)], small)

    @pl.when(serves)
    def _():
        landed(ranks.at[pl.ds(0, mates + 2 * (NEAR + 1))], small)

    @pl.when(is_second)
    def _():
        landed(ranks.at[pl.ds(0, mates + 1 + 2 * (NZ - 2 - NEAR))], small)

    @pl.when(is_end)
    def _():
        landed(ranks.at[pl.ds(0, mates + 1)], small)

    @pl.when(jnp.logical_not(edge_plane))
    def _():
        mine_to_root.wait_send()


def body(block_cols, step_tiles, mass, warm_start, source_ids):
    nx = lax.axis_size("patch_0")
    tile = step_tiles.shape[-1]
    rows, width = warm_start.shape
    edge, slots, square, sums = (2, tile, width), (3, tile, width), (tile, tile), (8, width)
    sem = pltpu.SemaphoreType.DMA
    return pl.pallas_call(
        functools.partial(kernel, nx, tile),
        out_shape=pltpu.VMEM((rows, width), F32),
        in_specs=[ANY] * 5,
        out_specs=pl.BlockSpec(memory_space=pltpu.VMEM),
        scratch_shapes=[
            pltpu.SMEM(block_cols.shape, jnp.int32),
            pltpu.VMEM((6, tile, tile), F32),
            pltpu.VMEM(mass.shape, F32),
            pltpu.VMEM((rows, width), F32),
            pltpu.VMEM(source_ids.shape, jnp.int32),
            pltpu.VMEM(slots, F32), pltpu.VMEM(slots, F32), pltpu.VMEM((5, *edge[1:]), F32),
            pltpu.VMEM(square, F32), pltpu.VMEM(edge[1:], F32),
            pltpu.VMEM(edge, F32), pltpu.VMEM((5, *edge[1:]), F32),
            pltpu.VMEM(square, F32), pltpu.VMEM(edge[1:], F32),
            pltpu.VMEM(sums, F32),
            pltpu.VMEM((2 * NZ - 4, *sums), F32),
            pltpu.VMEM(sums, F32),
            pltpu.VMEM((5 * nx, *sums), F32),
            pltpu.VMEM(sums, F32),
            sem((5,)),
            sem((3,)), sem((3,)),
            sem, sem, sem, sem, sem,
            pltpu.SemaphoreType.REGULAR,
            sem,
        ],
        compiler_params=pltpu.CompilerParams(collective_id=0, has_side_effects=True),
        name="heat",
    )(block_cols, step_tiles.reshape(6, tile, tile), mass, warm_start, source_ids)


def solution(mesh):
    split = Mesh(
        mesh.devices.reshape(mesh.shape["groups"], mesh.shape["patch"] // NZ, NZ, mesh.shape["sub"]), AXES
    )
    placed = (P(AXES, None), P(AXES, None, None, None), P(AXES), P(AXES, None), P("groups"))
    return jax.shard_map(body, mesh=split, in_specs=placed, out_specs=P(AXES, None), check_vma=False)
```

```python
import functools

import jax
import jax.numpy as jnp
from jax import lax
from jax.experimental import pallas as pl
from jax.experimental.pallas import tpu as pltpu
from jax.sharding import Mesh
from jax.sharding import PartitionSpec as P

NZ = 32
NEAR = 4
AXES = ("groups", "patch_0", "patch_1", "sub")
MESH = pl.DeviceIdType.MESH
F32, BF16 = jnp.float32, jnp.bfloat16
ANY = pl.BlockSpec(memory_space=pl.ANY)


def halves(value):
    high = value.astype(BF16)
    return high, (value - high.astype(F32)).astype(BF16)


def pair(value):
    return jnp.concatenate(halves(value), axis=1)


def product(high, low, packed):
    n = packed.shape[1] // 2
    both = jnp.dot(high, packed, preferred_element_type=F32)
    return both[:, :n] + (both[:, n:] + jnp.dot(low, packed[:, :n], preferred_element_type=F32))


def rows_sum(value):
    return jnp.sum(value, axis=0, keepdims=True)


def merged(buf):
    sq, cross, about, rss, quad, lin, curv = (buf[:, k, :] for k in range(7))
    sq_all, cross_all = rows_sum(sq), rows_sum(cross)
    centre = jnp.where(sq_all > 0, cross_all / sq_all, 0.0)
    off = about - centre
    first = cross - about * sq
    rss_all = rows_sum(rss + off * (2.0 * first + off * sq))
    quad_all = rows_sum(quad + off * (lin + off * curv))
    lin_all = rows_sum(lin + 2.0 * off * curv)
    return sq_all, cross_all, centre, rss_all, quad_all, lin_all, rows_sum(curv)


def kernel(
    nx, tile,
    cols_h, tiles_h, mass_h, x_h, src_h,
    out,
    cols, tiles, mass, x, src,
    halo_x, halo_s, halo_c, halo_m, halo_q, s_buf, c_buf, m_buf, q_buf, own, ranks, line, late, total,
    in_sem, x_rs, s_rs, m_rs, q_rs, y_rs, c_rs, z_rs, up_sem, l_rs,
):
    large, small, passing = in_sem.at[0], in_sem.at[1], in_sem.at[2]
    g, px, pz, pc = (lax.axis_index(name) for name in AXES)
    bar = pltpu.get_barrier_semaphore()

    def turn_x(d):
        return lax.rem(px + d + nx, nx)

    def turn_z(d):
        return lax.rem(pz + d + NZ, NZ)

    first, last = pz == 0, pz == NZ - 1
    right = (g, jnp.where((pc == 1) & last, turn_x(1), px), jnp.where(pc == 1, turn_z(1), pz), 1 - pc)
    left = (g, jnp.where((pc == 0) & first, turn_x(-1), px), jnp.where(pc == 0, turn_z(-1), pz), 1 - pc)
    far = tuple(jnp.where(pc == 1, a, b) for a, b in zip(right, left))
    partner = (g, px, pz, 1 - pc)
    is_root, is_caster, is_end = first & (pc == 1), first & (pc == 0), last & (pc == 1)
    by_way = (g, jnp.where(is_caster, turn_x(-1), left[1]), jnp.where(is_caster, 0, left[2]), left[3])
    way_slot = jnp.where(is_caster, 2, 1)

    loads = [
        pltpu.make_async_copy(a, b, in_sem.at[i])
        for i, (a, b) in enumerate(((x_h, x), (tiles_h, tiles), (mass_h, mass), (src_h, src), (cols_h, cols)))
    ]
    for load in loads:
        load.start()

    def greet(x_at, z_at, c_at):
        pl.semaphore_signal(bar, inc=1, device_id=(g, x_at, z_at, c_at), device_id_type=MESH)

    greet(*partner[1:])

    @pl.when(jnp.logical_not(is_end))
    def _():
        greet(*far[1:])

    @pl.when((pc == 1) & jnp.logical_not(first))
    def _():
        greet(px, pz - 1, 1)

    @pl.when(first)
    def _():
        for d in range(nx):
            for c in range(2):
                greet(turn_x(d), NZ - 1, c)
                if d > 0:
                    greet(turn_x(d), 0, c)

    @pl.when(is_root)
    def _():
        def greet_line(k, carry):
            greet(px, NZ - 1 - k, 0)
            greet(px, NZ - 1 - k, 1)
            return carry

        lax.fori_loop(1, NZ - 1, greet_line, 0)

    mates = 2 * nx - 1
    pl.semaphore_wait(
        bar, jnp.where(first, mates + 2 * pc, jnp.where(last, 2 + 2 * nx, 3 + pc))
    )

    def send(src, dst, ss, rs, to):
        pltpu.make_async_remote_copy(src, dst, ss, rs, device_id=to, device_id_type=MESH).start()

    def landed(ref, sem):
        pltpu.make_async_copy(ref, ref, sem).wait()

    @pl.when(is_end)
    def _():
        pl.semaphore_signal(up_sem, inc=1, device_id=(g, px, 0, 1), device_id_type=MESH)

    loads[0].wait()
    send(x.at[pl.ds(0, tile)], halo_x.at[way_slot], large, x_rs.at[way_slot], by_way)
    send(x.at[pl.ds(tile, tile)], halo_x.at[0], large, x_rs.at[0], right)
    for load in loads[1:]:
        load.wait()

    position = (px * NZ + pz) * 2 + pc
    parts = []
    for b in range(2):
        here = position * 2 + b
        found = []
        for d in (-1, 0, 1):
            found.append(sum((cols[b, k] == here + d).astype(F32) * tiles[3 * b + k] for k in range(3)))
        parts.append(found)
    (t0l, t00, t01), (t10, t11, t1r) = parts
    eye = lax.broadcasted_iota(jnp.int32, (tile, tile), 0) == lax.broadcasted_iota(jnp.int32, (tile, tile), 1)
    ones = jnp.ones((tile, tile), BF16)
    diag = []
    for b in range(2):
        row = mass[pl.ds(b * tile, tile)].reshape(1, tile)
        rest = jnp.where(eye, row, 0.0) + (parts[b][0] + parts[b][1] + parts[b][2])
        high = rest.astype(BF16)
        rest = rest - high.astype(F32)
        mid = rest.astype(BF16)
        low = (rest - mid.astype(F32)).astype(BF16)
        diag.append(sum(jnp.dot(part, ones, preferred_element_type=F32) for part in (low, mid, high)))
    diag_last = diag[1]
    diag = jnp.concatenate(diag, axis=0)
    inner = halves(jnp.concatenate([jnp.concatenate([t00, t01], axis=1), jnp.concatenate([t10, t11], axis=1)], axis=0))
    to_left, to_right = halves(t0l), halves(t1r)

    ceiling = 2.0 * jnp.max(diag, axis=0, keepdims=True)
    x_pair = pair(x[...])
    ids = lax.broadcasted_iota(jnp.int32, (2 * tile, src.shape[0]), 0) + position * 2 * tile
    rhs = (ids == src[...].reshape(1, -1)).astype(F32)
    s = rhs - diag * x[...] + product(*inner, x_pair)
    s_buf[0] = s[:tile]
    s_buf[1] = s[tile:]
    m_buf[...] = jnp.where(eye, diag_last, 0.0) - t11
    from_left, from_right = halves(t0l.T), halves(t1r.T)
    send(s_buf.at[0], halo_s.at[way_slot], large, s_rs.at[way_slot], by_way)
    send(s_buf.at[1], halo_s.at[0], large, s_rs.at[0], right)
    to_chip = [
        pltpu.make_async_remote_copy(src, dst, large, rs, device_id=(*right[:3], 1), device_id_type=MESH)
        for src, dst, rs in ((m_buf, halo_m, m_rs), (q_buf, halo_q, q_rs))
    ]
    to_core = [
        pltpu.make_async_remote_copy(
            c_buf.at[i], halo_c.at[i], passing, y_rs if i == 4 else c_rs, device_id=partner, device_id_type=MESH
        )
        for i in range(5)
    ]

    passed = [
        pltpu.make_async_remote_copy(
            ref.at[2], ref.at[1], passing, rs.at[1], device_id=(g, px, NZ - 1, 1), device_id_type=MESH
        )
        for ref, rs in ((halo_x, x_rs), (halo_s, s_rs))
    ]

    @pl.when(is_root)
    def _():
        landed(halo_x.at[2], x_rs.at[2])
        landed(halo_s.at[2], s_rs.at[2])
        pl.semaphore_wait(up_sem, 1)
        for copy in passed:
            copy.start()

    @pl.when(pc == 1)
    def _():
        to_chip[0].start()
        landed(halo_x.at[0], x_rs.at[0])
        behind = s[:tile] + product(*to_left, pair(halo_x[0]))
        whole = jnp.concatenate([behind, s[tile:]], axis=0)
        q_buf[...] = diag_last * s[tile:] - product(inner[0][tile:], inner[1][tile:], pair(whole))
        to_chip[1].start()

    on_left = product(*from_left, x_pair[:tile])
    on_right = product(*from_right, x_pair[tile:])

    @pl.when(pc == 0)
    def _():
        c_buf[4] = on_left
        to_core[4].start()
        landed(halo_x.at[0], x_rs.at[0])

    landed(halo_x.at[1], x_rs.at[1])
    r = s + jnp.concatenate([product(*to_left, pair(halo_x[0])), product(*to_right, pair(halo_x[1]))], axis=0)
    r_pair = pair(r)
    near_r = diag * r - product(*inner, r_pair)
    back_r = product(*from_left, r_pair[:tile])
    landed(halo_s.at[0], s_rs.at[0])
    landed(halo_s.at[1], s_rs.at[1])
    next_r = [halo_s[0] + on_left, halo_s[1] + on_right]
    w = near_r - jnp.concatenate([product(*to_left, pair(next_r[0])), product(*to_right, pair(next_r[1]))], axis=0)

    @pl.when(pc == 0)
    def _():
        for i, value in enumerate((w[tile:], back_r, next_r[0])):
            c_buf[i] = value
            to_core[i].start()

    w_pair = pair(w)
    sq, cross = rows_sum(r * r), rows_sum(r * w)
    about = jnp.where(sq > 0, jnp.clip(cross / sq, 0.0, ceiling), 0.0)
    u = w - about * r
    rss = rows_sum(u * u)
    near_u = diag * w - product(*inner, w_pair) - about * near_r
    back_w = product(*from_left, w_pair[:tile])

    @pl.when(pc == 0)
    def _():
        c_buf[3] = back_w
        to_core[3].start()

    quad, lin, curv = rows_sum(u * near_u), 2.0 * rows_sum(r * near_u), rows_sum(r * near_r)

    own[...] = jnp.concatenate([sq, cross, about, rss, quad, lin, curv, jnp.zeros_like(sq)], axis=0)

    @pl.when(pc == 1)
    def _():
        landed(halo_c.at[4], y_rs)
        landed(halo_m, m_rs)
        across_m = product(*halves(halo_m[...]), pair(halo_c[4]))
        landed(halo_q, q_rs)
        landed(halo_c.at[pl.ds(0, 4)], c_rs)
        w_at, back_r_at, next_r_at, back_w_at = (halo_c[i] for i in range(4))
        quads, lins, curvs = quad, lin, curv
        for edge_w, edge_r, edge_back_w, edge_back_r in (
            (w_at, next_r[0], back_w, back_r),
            (halo_q[...] + across_m - back_r_at, next_r_at, back_w_at, back_r_at),
        ):
            edge_u, edge_back_u = edge_w - about * edge_r, edge_back_w - about * edge_back_r
            quads -= 2.0 * rows_sum(edge_back_u * edge_u)
            lins -= 2.0 * rows_sum(edge_back_u * edge_r + edge_back_r * edge_u)
            curvs -= 2.0 * rows_sum(edge_back_r * edge_r)
        own[...] = jnp.concatenate([sq, cross, about, rss, quads, lins, curvs, jnp.zeros_like(sq)], axis=0)

    blank = jnp.zeros((1, sq.shape[1]), F32)

    edge_plane = first | last
    slot = jnp.where(edge_plane, nx + jnp.where(first, 2 * nx, 0) + px * 2 + pc, 0)
    rank = jnp.where(edge_plane, 0, (pz - 1) * 2 + pc)
    others = [(d, c) for d in (2, 1, nx - 1, 0) for c in range(2) if (d, c) != (0, 0)]

    def share(src, at, targets):
        return [
            pltpu.make_async_remote_copy(
                src, late.at[at], small, l_rs, device_id=(g, turn_x(d), 0, lax.rem(pc + c, 2)), device_id_type=MESH
            )
            for d, c in targets
        ]

    mine_out, line_out = share(own, slot, others), share(line, px, others)
    (mine_down,) = share(own, slot, [(0, 0)])
    mine_to_root = pltpu.make_async_remote_copy(
        own, ranks.at[rank], small, z_rs, device_id=(g, px, 0, 1), device_id_type=MESH
    )

    @pl.when(edge_plane)
    def _():
        for copy in mine_out:
            copy.start()

    @pl.when(last)
    def _():
        mine_down.start()

    @pl.when(jnp.logical_not(edge_plane))
    def _():
        mine_to_root.start()

    count = 5 * nx

    @pl.when(is_root)
    def _():
        inner_planes = ranks.at[pl.ds(0, 2 * NZ - 4)]
        landed(inner_planes, z_rs)
        joined = jnp.concatenate([*merged(inner_planes), blank], axis=0)
        line[...] = joined
        for copy in line_out:
            copy.start()
        late[px] = joined
        late[slot] = own[...]
        landed(late.at[pl.ds(0, count - 2)], l_rs)

    @pl.when(is_caster)
    def _():
        late[slot] = own[...]
        landed(late.at[pl.ds(0, count - 1)], l_rs)

    def to_chip_at(k, x_at=px):
        return [
            pltpu.make_async_remote_copy(total, total, small, l_rs, device_id=(g, x_at, k, c), device_id_type=MESH)
            for c in (1, 0)
        ]

    @pl.when(first)
    def _():
        sq, cross, _, rss, quad, _, _ = merged(late.at[pl.ds(0, count)])
        step = sq / cross
        after = step * step * rss
        ratio = after / sq
        step_next = after / (step * step * quad - ratio * after / step)
        total[...] = jnp.concatenate(
            [step + step_next * (1.0 + ratio), -(step_next * step), jnp.zeros((6, sq.shape[1]), F32)], axis=0
        )

    @pl.when(jnp.logical_not(first))
    def _():
        landed(total, l_rs)

    is_second = last & (pc == 0)
    serves, is_server = is_caster & (px > 0), is_root & (px == nx - 1)

    @pl.when(serves | is_server)
    def _():
        for k in (*range(1, NEAR + 1), NZ - 1):
            for copy in to_chip_at(k, jnp.where(is_server, 0, px)):
                copy.start()

    @pl.when(is_second)
    def _():
        def step(k, carry):
            for copy in to_chip_at(k):
                copy.start()
            return carry

        lax.fori_loop(NEAR + 1, NZ - 1, step, 0)

    out[...] = x[...] + total[0:1] * r + total[1:2] * w

    @pl.when(pc == 0)
    def _():
        landed(tiles.at[pl.ds(0, 4)], large)
        landed(tiles.at[pl.ds(0, 5)], passing)

    @pl.when(pc == 1)
    def _():
        landed(tiles, large)

    @pl.when(is_root)
    def _():
        landed(halo_x.at[pl.ds(0, 2)], passing)

    @pl.when(is_root & (px < nx - 1))
    def _():
        landed(ranks.at[pl.ds(0, 2 * mates)], small)

    @pl.when(is_server)
    def _():
        landed(ranks.at[pl.ds(0, 2 * mates + 2 * (NEAR + 1))], small)

    @pl.when(is_caster & (px == 0))
    def _():
        landed(ranks.at[pl.ds(0, mates)], small)

    @pl.when(serves)
    def _():
        landed(ranks.at[pl.ds(0, mates + 2 * (NEAR + 1))], small)

    @pl.when(is_second)
    def _():
        landed(ranks.at[pl.ds(0, mates + 1 + 2 * (NZ - 2 - NEAR))], small)

    @pl.when(is_end)
    def _():
        landed(ranks.at[pl.ds(0, mates + 1)], small)

    @pl.when(jnp.logical_not(edge_plane))
    def _():
        mine_to_root.wait_send()


def body(block_cols, step_tiles, mass, warm_start, source_ids):
    nx = lax.axis_size("patch_0")
    tile = step_tiles.shape[-1]
    rows, width = warm_start.shape
    edge, slots, square, sums = (2, tile, width), (3, tile, width), (tile, tile), (8, width)
    sem = pltpu.SemaphoreType.DMA
    return pl.pallas_call(
        functools.partial(kernel, nx, tile),
        out_shape=pltpu.VMEM((rows, width), F32),
        in_specs=[ANY] * 5,
        out_specs=pl.BlockSpec(memory_space=pltpu.VMEM),
        scratch_shapes=[
            pltpu.SMEM(block_cols.shape, jnp.int32),
            pltpu.VMEM((6, tile, tile), F32),
            pltpu.VMEM(mass.shape, F32),
            pltpu.VMEM((rows, width), F32),
            pltpu.VMEM(source_ids.shape, jnp.int32),
            pltpu.VMEM(slots, F32), pltpu.VMEM(slots, F32), pltpu.VMEM((5, *edge[1:]), F32),
            pltpu.VMEM(square, F32), pltpu.VMEM(edge[1:], F32),
            pltpu.VMEM(edge, F32), pltpu.VMEM((5, *edge[1:]), F32),
            pltpu.VMEM(square, F32), pltpu.VMEM(edge[1:], F32),
            pltpu.VMEM(sums, F32),
            pltpu.VMEM((2 * NZ, *sums), F32),
            pltpu.VMEM(sums, F32),
            pltpu.VMEM((6 * nx, *sums), F32),
            pltpu.VMEM(sums, F32),
            sem((5,)),
            sem((3,)), sem((3,)),
            sem, sem, sem, sem, sem,
            pltpu.SemaphoreType.REGULAR,
            sem,
        ],
        compiler_params=pltpu.CompilerParams(collective_id=0, has_side_effects=True),
        name="heat",
    )(block_cols, step_tiles.reshape(6, tile, tile), mass, warm_start, source_ids)


def solution(mesh):
    split = Mesh(
        mesh.devices.reshape(mesh.shape["groups"], mesh.shape["patch"] // NZ, NZ, mesh.shape["sub"]), AXES
    )
    placed = (P(AXES, None), P(AXES, None, None, None), P(AXES), P(AXES, None), P("groups"))
    return jax.shard_map(body, mesh=split, in_specs=placed, out_specs=P(AXES, None), check_vma=False)
```
